512 devices in a mesh: gx: 8 (over z_lo, x), gy: 4 (over z_hi), gz: 16 (over y, core).
Axes of the slice: x: 4, y: 8, z: 8 (z_hi: 4, z_lo: 2; z = z_hi * 2 + z_lo), core: 2. Of those that a mesh axis runs over, the one named last changes fastest.
Arguments:
- vectors: float32 [3, 48, 24, 96, 128], P(None, 'gx', 'gy', 'gz'), may hold values from -6 to 6
- orient_flip: int32 [16, 8, 4608], P('gx', 'gy', 'gz'), may hold values from 0 to 1
- reluctivity: float32 [16, 8, 2048], P('gx', 'gy', 'gz'), may hold values from 0.05 to 0.5
- conductivity: float32 [16, 8, 2048], P('gx', 'gy', 'gz'), may hold values from 1 to 10
Outputs:
- out_x: float32 [48, 28, 112, 128], P('gx', 'gy', 'gz')
- out_y: float32 [56, 24, 112, 128], P('gx', 'gy', 'gz')
- out_z: float32 [56, 28, 96, 128], P('gx', 'gy', 'gz')
The draws below stay inside these ranges and needn't reach their ends.
Inputs may be any that keep to these rules, and one draw needn't show every extreme that they name: `orient_flip`: 1 reverses the orientation of that degree of freedom in that element, 0 keeps it.
All inputs are finite; a program needn't handle non-finite values.
Results may differ from the reference program's by a relative error of at most 0.00007.
Values sent between devices are 32-bit elements; how exact they have to be, the bound alone decides.
A program may use at most 64 MiB of HBM per device.

```python
import math
import jax
import jax.numpy as jnp
import numpy as np
from jax import lax

ORDER = 3
QUAD = 4
VECS = 128
NX = 16
NY = 8
NZ = 32
ELEM_DOFS = 144
QPTS = 64
N_GX = 8
N_GY = 4
N_GZ = 16


def touch_ends(entries, key, low, high):
    place = [jax.random.randint(jax.random.fold_in(key, axis), (), 0, length) for axis, length in enumerate(entries.shape)]
    widest = entries.shape.index(max(entries.shape))
    neighbour = place[:widest] + [(place[widest] + 1) % entries.shape[widest]] + place[widest + 1:]
    return entries.at[tuple(place)].set(low).at[tuple(neighbour)].set(high)


def levels(key, shape, shards, least, largest):
    gain, own = 1.0, jax.random.fold_in(key, 6)
    for axis_at, parts in shards:
        heights = jnp.exp(jax.random.uniform(jax.random.fold_in(own, axis_at), (parts,), jnp.float32, least / len(shards), largest / len(shards)))
        gain = gain * jnp.repeat(heights, shape[axis_at] // parts).reshape([-1 if axis == axis_at else 1 for axis in range(len(shape))])
    return gain


def scatter_about(own_key, shape, scale, most, pieces=(), kind=jnp.bfloat16):
    entries = jax.random.normal(own_key, shape, jnp.float32) * scale
    if len(pieces) > 0:
        entries = levels(own_key, shape, pieces, -0.22, 0.18) * entries
    return jnp.clip(entries, min=-most, max=most).astype(kind)


def setup_inputs(seed: int = 0) -> dict:
    key_of = jax.random.split(jax.random.key(seed), 5)
    vectors = scatter_about(key_of[0], (3, NX * ORDER, NY * ORDER, NZ * ORDER, VECS), 1.0, 6.0, ((1, 8), (2, 4), (3, 16)), jnp.float32)
    orient_flip = touch_ends(jax.random.randint(key_of[1], (NX, NY, NZ * ELEM_DOFS), 0, 2), jax.random.fold_in(key_of[1], 1), 0, 1).astype(jnp.int32)
    reluctivity = jnp.clip(jnp.exp(math.log(0.5) - 2.3025851 * jax.random.uniform(key_of[2], (NX, NY, NZ * QPTS), jnp.float32) ** levels(key_of[2], (NX, NY, NZ * QPTS), ((0, 8), (1, 4), (2, 16)), -0.2, 0.2)), 0.05, 0.5)
    conductivity = jnp.clip(jnp.exp(math.log(10.0) - 2.3025851 * jax.random.uniform(key_of[3], (NX, NY, NZ * QPTS), jnp.float32) ** levels(key_of[3], (NX, NY, NZ * QPTS), ((0, 8), (1, 4), (2, 16)), -0.2, 0.2)), 1.0, 10.0)
    return {"vectors": vectors, "orient_flip": orient_flip, "reluctivity": reluctivity, "conductivity": conductivity}


def lagrange(points_at, evaluate_at):
    amount = len(points_at)
    values = np.ones((len(evaluate_at), amount))
    slopes = np.zeros((len(evaluate_at), amount))
    for which in range(amount):
        for column in range(amount):
            if column != which:
                factor = (evaluate_at - points_at[column]) / (points_at[which] - points_at[column])
                slopes[:, which] = slopes[:, which] * factor + values[:, which] / (points_at[which] - points_at[column])
                values[:, which] = values[:, which] * factor
    return (values, slopes)

def basis_tables():
    lobatto = np.array([0.0, (1 - 5 ** (-0.5)) / 2, (1 + 5 ** (-0.5)) / 2, 1.0])
    gauss_open = np.array([(1 - 0.6 ** 0.5) / 2, 0.5, (1 + 0.6 ** 0.5) / 2])
    inner_pt = (3.0 / 7 - 2.0 / 7 * (6.0 / 5) ** 0.5) ** 0.5
    outer_pt = (3.0 / 7 + 2.0 / 7 * (6.0 / 5) ** 0.5) ** 0.5
    inner_wt = (18 + 30 ** 0.5) / 36
    outer_wt = (18 - 30 ** 0.5) / 36
    quad_points = (1 + np.array([-outer_pt, -inner_pt, inner_pt, outer_pt])) / 2
    quad_weight = np.array([outer_wt, inner_wt, inner_wt, outer_wt]) / 2
    closed, slopes = lagrange(lobatto, quad_points)
    opened, unused_slopes = lagrange(gauss_open, quad_points)
    weight_cube = quad_weight[:, None, None, None, None] * quad_weight[None, :, None, None, None] * quad_weight[None, None, :, None, None]
    return (jnp.asarray(closed, dtype=jnp.float32), jnp.asarray(slopes, dtype=jnp.float32), jnp.asarray(opened, dtype=jnp.float32), jnp.asarray(weight_cube, dtype=jnp.float32))

def contract(tensor, first_mat, second_mat, third_mat):
    section_one = jnp.einsum('qa,abcef->qbcef', first_mat, tensor, precision=lax.Precision.HIGHEST)
    section_two = jnp.einsum('rb,qbcef->qrcef', second_mat, section_one, precision=lax.Precision.HIGHEST)
    return jnp.einsum('sc,qrcef->qrsef', third_mat, section_two, precision=lax.Precision.HIGHEST)

def evaluate(elem_x, elem_y, elem_z, closed, slopes, opened):
    u_x = contract(elem_x, opened, closed, closed)
    u_y = contract(elem_y, closed, opened, closed)
    u_z = contract(elem_z, closed, closed, opened)
    deriv_xy = contract(elem_x, opened, slopes, closed)
    deriv_xz = contract(elem_x, opened, closed, slopes)
    deriv_yx = contract(elem_y, slopes, opened, closed)
    deriv_yz = contract(elem_y, closed, opened, slopes)
    deriv_zx = contract(elem_z, slopes, closed, opened)
    deriv_zy = contract(elem_z, closed, slopes, opened)
    return (u_x, u_y, u_z, deriv_zy - deriv_yz, deriv_xz - deriv_zx, deriv_yx - deriv_xy)

def windows(array, axis, amount, open_dim):
    dims_now = array.shape
    if open_dim:
        split = array.reshape(dims_now[:axis] + (amount, ORDER) + dims_now[axis + 1:])
        return jnp.swapaxes(split, axis, axis + 1)
    reach = ORDER * (amount - 1) + 1
    return jnp.stack([lax.slice_in_dim(array, offset, offset + reach, ORDER, axis) for offset in range(ORDER + 1)], axis=axis)

def collect(array, open_axis, counts):
    result = array
    for axis in range(3):
        result = windows(result, 2 * axis, counts[axis], axis == open_axis)
    dims_now = result.shape
    result = jnp.transpose(result, (0, 2, 4, 1, 3, 5, 6))
    return result.reshape(dims_now[0], dims_now[2], dims_now[4], counts[0] * counts[1] * counts[2], dims_now[6])

def element_data(orient_flip, reluctivity, conductivity, elements):
    flip_float = orient_flip.reshape(elements, ELEM_DOFS).T.astype(jnp.float32)
    sign_all = 1.0 - 2.0 * flip_float
    per_comp = ORDER * (ORDER + 1) * (ORDER + 1)
    sign_x = sign_all[:per_comp].reshape(ORDER, ORDER + 1, ORDER + 1, elements, 1)
    sign_y = sign_all[per_comp:2 * per_comp].reshape(ORDER + 1, ORDER, ORDER + 1, elements, 1)
    sign_z = sign_all[2 * per_comp:].reshape(ORDER + 1, ORDER + 1, ORDER, elements, 1)
    reluct = reluctivity.reshape(elements, QPTS).T.reshape(QUAD, QUAD, QUAD, elements, 1)
    conduct = conductivity.reshape(elements, QPTS).T.reshape(QUAD, QUAD, QUAD, elements, 1)
    return (sign_x, sign_y, sign_z, reluct, conduct)

def element_apply(lvec_x, lvec_y, lvec_z, data, counts):

    def gather_all(part_x, part_y, part_z):
        return (collect(part_x, 0, counts), collect(part_y, 1, counts), collect(part_z, 2, counts))
    elems, scatter_back = jax.vjp(gather_all, lvec_x, lvec_y, lvec_z)
    sign_x, sign_y, sign_z, reluct, conduct = data
    closed, slopes, opened, weight_cube = basis_tables()

    def forward(part_x, part_y, part_z):
        return evaluate(part_x, part_y, part_z, closed, slopes, opened)
    quads, pullback = jax.vjp(forward, elems[0] * sign_x, elems[1] * sign_y, elems[2] * sign_z)
    mass_scale = weight_cube * conduct
    curl_scale = weight_cube * reluct
    cotangent = (mass_scale * quads[0], mass_scale * quads[1], mass_scale * quads[2], curl_scale * quads[3], curl_scale * quads[4], curl_scale * quads[5])
    grads = pullback(cotangent)
    return scatter_back((grads[0] * sign_x, grads[1] * sign_y, grads[2] * sign_z))

def extend(array, axes):
    for axis in axes:
        array = jnp.concatenate([array, lax.slice_in_dim(array, 0, 1, 1, axis)], axis)
    return array

def fold_back(array, axes):
    for axis in axes:
        total_len = array.shape[axis]
        head_sum = lax.slice_in_dim(array, 0, 1, 1, axis) + lax.slice_in_dim(array, total_len - 1, total_len, 1, axis)
        array = jnp.concatenate([head_sum, lax.slice_in_dim(array, 1, total_len - 1, 1, axis)], axis)
    return array

def spread(array, axis, blocks):
    dims_now = array.shape
    block_len = dims_now[axis] // blocks
    split = array.reshape(dims_now[:axis] + (blocks, block_len) + dims_now[axis + 1:])
    following = jnp.roll(lax.slice_in_dim(split, 0, 1, 1, axis + 1), -1, axis)
    joined = jnp.concatenate([split, following], axis + 1)
    return joined.reshape(dims_now[:axis] + (blocks * (block_len + 1),) + dims_now[axis + 1:])

def reference(vectors, orient_flip, reluctivity, conductivity):
    data = element_data(orient_flip, reluctivity, conductivity, NX * NY * NZ)
    group = math.gcd(VECS, 2)
    dims_now = vectors.shape
    grouped = jnp.moveaxis(vectors.reshape(dims_now[:4] + (VECS // group, group)), 4, 0)

    def apply_whole(single):
        results = element_apply(extend(single[0], (1, 2)), extend(single[1], (0, 2)), extend(single[2], (0, 1)), data, (NX, NY, NZ))
        own_x = fold_back(results[0], (1, 2))
        own_y = fold_back(results[1], (0, 2))
        own_z = fold_back(results[2], (0, 1))
        return (spread(spread(own_x, 1, N_GY), 2, N_GZ), spread(spread(own_y, 0, N_GX), 2, N_GZ), spread(spread(own_z, 0, N_GX), 1, N_GY))
    parts_x, parts_y, parts_z = lax.map(apply_whole, grouped)

    def unite(stacked):
        moved = jnp.moveaxis(stacked, 0, 3)
        shape_now = moved.shape
        return moved.reshape(shape_now[:3] + (VECS,))
    return (unite(parts_x), unite(parts_y), unite(parts_z))
```

```python
import jax
import jax.numpy as jnp
import numpy as np
from jax import lax
from jax.experimental import pallas as pl
from jax.experimental.pallas import tpu as pltpu
from jax.sharding import PartitionSpec as P

MESH = pl.DeviceIdType.MESH
AXES = ("gx", "gy", "gz")
LANES = 128
DOFS = 144
QPTS = 64
BASE = (0, 48, 96)
STRIDE = ((16, 4, 1), (12, 4, 1), (12, 3, 1))
EDGE_AXES = ((1, 2), (0, 2), (0, 1))
FACE_COMPS = ((1, 2), (0, 2), (0, 1))
SIGNS = ((-1, -1), (-1, 1), (1, -1), (1, 1))


def lagrange(points_at, evaluate_at):
    amount = len(points_at)
    values = np.ones((len(evaluate_at), amount))
    slopes = np.zeros((len(evaluate_at), amount))
    for which in range(amount):
        for column in range(amount):
            if column != which:
                factor = (evaluate_at - points_at[column]) / (points_at[which] - points_at[column])
                slopes[:, which] = slopes[:, which] * factor + values[:, which] / (
                    points_at[which] - points_at[column]
                )
                values[:, which] = values[:, which] * factor
    return (values, slopes)


def basis_tables():
    lobatto = np.array([0.0, (1 - 5 ** (-0.5)) / 2, (1 + 5 ** (-0.5)) / 2, 1.0])
    gauss_open = np.array([(1 - 0.6**0.5) / 2, 0.5, (1 + 0.6**0.5) / 2])
    inner_pt = (3.0 / 7 - 2.0 / 7 * (6.0 / 5) ** 0.5) ** 0.5
    outer_pt = (3.0 / 7 + 2.0 / 7 * (6.0 / 5) ** 0.5) ** 0.5
    inner_wt = (18 + 30**0.5) / 36
    outer_wt = (18 - 30**0.5) / 36
    quad_points = (1 + np.array([-outer_pt, -inner_pt, inner_pt, outer_pt])) / 2
    quad_weight = np.array([outer_wt, inner_wt, inner_wt, outer_wt]) / 2
    closed, slopes = lagrange(lobatto, quad_points)
    opened, unused_slopes = lagrange(gauss_open, quad_points)
    return (closed, slopes, opened, quad_weight)


CLOSED, SLOPES, OPENED, WEIGHT = basis_tables()
DERIV = SLOPES @ np.linalg.inv(CLOSED)


def apply(table, given, parity):
    rows, columns = table.shape
    half = columns // 2
    sums = [given[c] + given[columns - 1 - c] for c in range(half)]
    diffs = [given[c] - given[columns - 1 - c] for c in range(half)]
    result = [None] * rows
    for q in range((rows + 1) // 2):
        even = None
        for c in range(half):
            term = sums[c] * float((table[q, c] + table[q, columns - 1 - c]) / 2)
            even = term if even is None else even + term
        if columns % 2:
            even = even + given[half] * float(table[q, half])
        if 2 * q + 1 == rows:
            result[q] = even
            continue
        odd = None
        for c in range(half):
            term = diffs[c] * float((table[q, c] - table[q, columns - 1 - c]) / 2)
            odd = term if odd is None else odd + term
        result[q] = even + odd
        result[rows - 1 - q] = even - odd if parity > 0 else odd - even
    return result


def along_rows(table, plane, parity=1):
    columns = [apply(table, [row[c] for row in plane], parity) for c in range(len(plane[0]))]
    return [[column[q] for column in columns] for q in range(table.shape[0])]


def along_columns(table, plane, parity=1):
    return [apply(table, row, parity) for row in plane]


def combine(op, *planes):
    return [[op(*entries) for entries in zip(*rows)] for rows in zip(*planes)]


def plus(p, q):
    return combine(lambda s, t: s + t, p, q)


def minus(p, q):
    return combine(lambda s, t: s - t, p, q)


def times(p, q):
    return combine(lambda s, t: s * t, p, q)


def dof(comp, a, b, c):
    s = STRIDE[comp]
    return BASE[comp] + a * s[0] + b * s[1] + c * s[2]


def row_of(comp, a, b, c, element=0):
    return 8 * dof(comp, a, b, c) + element


def element(i, j, k):
    return 4 * k + 2 * i + j


def places(comp, axis):
    if comp == axis:
        return [(g, g // 3, g % 3) for g in range(6)]
    return [(g, 0, g) for g in range(4)] + [(g, 1, g - 3) for g in range(3, 7)]


def owners(comp, axis):
    last = 6 if comp == axis else 7
    return [(g, min(g // 3, 1), g - 3 * min(g // 3, 1)) for g in range(last)]


def prepare(flip, rel, con, flat, sign, mass, curl):
    for k in range(2):
        for i in range(2):
            at = pl.ds(4 * k + 2 * i, 2)
            flat[at, 0:DOFS] = 1.0 - 2.0 * flip[i][:, DOFS * k : DOFS * (k + 1)].astype(jnp.float32)
            flat[at, 256 : 256 + QPTS] = rel[i][:, QPTS * k : QPTS * (k + 1)]
            flat[at, 384 : 384 + QPTS] = con[i][:, QPTS * k : QPTS * (k + 1)]
    whole = flat[:, 0:DOFS]
    for d in range(DOFS):
        sign[d] = jnp.broadcast_to(whole[:, d : d + 1], (8, LANES))
    rel_all = flat[:, 256 : 256 + QPTS]
    con_all = flat[:, 384 : 384 + QPTS]
    for q in range(QPTS):
        weight = float(WEIGHT[q // 16] * WEIGHT[q // 4 % 4] * WEIGHT[q % 4])
        curl[q] = jnp.broadcast_to(rel_all[:, q : q + 1], (8, LANES)) * weight
        mass[q] = jnp.broadcast_to(con_all[:, q : q + 1], (8, LANES)) * weight


def compute(dofs, sign, mass, curl, temp, u_x, u_y, c_x, c_y, c_z):
    def load(d):
        return dofs[pl.ds(pl.multiple_of(8 * d, 8), 8), :] * sign[d]

    def store(d, value):
        dofs[pl.ds(pl.multiple_of(8 * d, 8), 8), :] = value * sign[d]

    def quad(x, y, z):
        return 16 * x + 4 * y + z

    four = range(4)

    def planes(ref, at):
        return [[ref[at(p, q)] for q in four] for p in four]

    def put(ref, at, plane):
        for p in four:
            for q in four:
                ref[at(p, q)] = plane[p][q]

    @pl.loop(0, 4)
    def _(b):
        for c in four:
            values = apply(OPENED, [load(dof(0, a, b, c)) for a in range(3)], 1)
            for q in four:
                temp[quad(q, b, c)] = values[q]

    @pl.loop(0, 4)
    def _(x):
        at = lambda y, z: quad(x, y, z)
        u = along_columns(CLOSED, along_rows(CLOSED, planes(temp, at)))
        put(u_x, at, u)
        put(c_z, at, along_rows(-DERIV, u, -1))
        put(c_y, at, along_columns(DERIV, u, -1))

    @pl.loop(0, 4)
    def _(a):
        values = [[load(dof(1, a, b, c)) for c in four] for b in range(3)]
        put(temp, lambda y, z: quad(a, y, z), along_columns(CLOSED, along_rows(OPENED, values)))

    @pl.loop(0, 4)
    def _(y):
        at = lambda x, z: quad(x, y, z)
        u = along_rows(CLOSED, planes(temp, at))
        put(u_y, at, u)
        put(c_z, at, plus(planes(c_z, at), along_rows(DERIV, u, -1)))
        put(c_x, at, along_columns(-DERIV, u, -1))

    @pl.loop(0, 4)
    def _(a):
        values = [[load(dof(2, a, b, c)) for c in range(3)] for b in four]
        put(temp, lambda y, z: quad(a, y, z), along_rows(CLOSED, along_columns(OPENED, values)))

    @pl.loop(0, 4)
    def _(z):
        at = lambda x, y: quad(x, y, z)
        u = along_rows(CLOSED, planes(temp, at))
        scale = planes(curl, at)
        w_y = times(scale, minus(planes(c_y, at), along_rows(DERIV, u, -1)))
        w_x = times(scale, plus(planes(c_x, at), along_columns(DERIV, u, -1)))
        put(c_y, at, w_y)
        put(c_x, at, w_x)
        v = times(planes(mass, at), u)
        v = plus(v, along_columns(DERIV.T, w_x, -1))
        v = minus(v, along_rows(DERIV.T, w_y, -1))
        put(temp, at, along_rows(CLOSED.T, v))

    @pl.loop(0, 4)
    def _(a):
        values = along_rows(CLOSED.T, planes(temp, lambda y, z: quad(a, y, z)))
        values = along_columns(OPENED.T, values)
        for b in four:
            for c in range(3):
                store(dof(2, a, b, c), values[b][c])

    @pl.loop(0, 4)
    def _(y):
        at = lambda x, z: quad(x, y, z)
        w_z = times(planes(curl, at), planes(c_z, at))
        put(c_z, at, w_z)
        v = times(planes(mass, at), planes(u_y, at))
        v = plus(v, along_rows(DERIV.T, w_z, -1))
        v = minus(v, along_columns(DERIV.T, planes(c_x, at), -1))
        put(temp, at, along_rows(CLOSED.T, v))

    @pl.loop(0, 4)
    def _(a):
        values = along_columns(CLOSED.T, planes(temp, lambda y, z: quad(a, y, z)))
        values = along_rows(OPENED.T, values)
        for b in range(3):
            for c in four:
                store(dof(1, a, b, c), values[b][c])

    @pl.loop(0, 4)
    def _(x):
        at = lambda y, z: quad(x, y, z)
        v = times(planes(mass, at), planes(u_x, at))
        v = plus(v, along_columns(DERIV.T, planes(c_y, at), -1))
        v = minus(v, along_rows(DERIV.T, planes(c_z, at), -1))
        put(temp, at, along_rows(CLOSED.T, along_columns(CLOSED.T, v)))

    @pl.loop(0, 4)
    def _(b):
        for c in four:
            values = apply(OPENED.T, [temp[quad(q, b, c)] for q in four], 1)
            for a in range(3):
                store(dof(0, a, b, c), values[a])


def join_elements(dofs):
    rows = lax.broadcasted_iota(jnp.int32, (8, LANES), 0)
    for axis, step in ((0, 2), (1, 1), (2, 4)):
        upper = (rows // step) % 2 == 1
        for comp in range(3):
            if comp == axis:
                continue
            sizes = [3 if comp == other else 4 for other in range(3)]
            sizes[axis] = 1
            for a in range(sizes[0]):
                for b in range(sizes[1]):
                    for c in range(sizes[2]):
                        low = [a, b, c]
                        high = [a, b, c]
                        high[axis] = 3
                        to = pl.ds(row_of(comp, *low), 8)
                        moved = pltpu.roll(dofs[pl.ds(row_of(comp, *high), 8), :], step, 0)
                        dofs[to, :] = dofs[to, :] + jnp.where(upper, moved, 0.0)


def scatter_own(vec, dofs):
    for comp in range(3):
        for x, i, a in places(comp, 0):
            for y, j, b in places(comp, 1):
                if x == 6 or y == 6:
                    continue
                for k in range(2):
                    count = 4 if comp != 2 and k == 0 else 3
                    at = row_of(comp, a, b, 0, element(i, j, k))
                    dofs[pl.ds(at, count, 8), :] = vec[comp, x, y, pl.ds(3 * k, count), :]


def scatter_halo(dofs, r_x, r_y, r_z, r_e):
    def line(comp, i, a, j, b, source):
        for k in range(2):
            count = 4 if comp != 2 and k == 0 else 3
            at = row_of(comp, a, b, 0, element(i, j, k))
            dofs[pl.ds(at, count, 8), :] = source(pl.ds(3 * k, count))

    for comp in (1, 2):
        for y, j, b in places(comp, 1):
            if y < 6:
                line(comp, 1, 3, j, b, lambda z: r_x[comp - 1, y, z, :])
    for comp in (0, 2):
        for x, i, a in places(comp, 0):
            if x < 6:
                line(comp, i, a, 1, 3, lambda z: r_y[comp // 2, x, z, :])
    line(2, 1, 3, 1, 3, lambda z: r_e[2, z, :])
    for x, i, a in places(0, 0):
        for j in range(2):
            count = 4 - j
            at = row_of(0, a, 0, 3, element(i, j, 1))
            dofs[pl.ds(at, count, 32), :] = r_z[0, x, pl.ds(3 * j, count), :]
    for x, i, a in places(1, 0):
        if x < 6:
            for j in range(2):
                at = row_of(1, a, 0, 3, element(i, j, 1))
                dofs[pl.ds(at, 3, 32), :] = r_z[1, x, pl.ds(3 * j, 3), :]
    for i in range(2):
        at = row_of(0, 0, 3, 3, element(i, 1, 1))
        dofs[pl.ds(at, 3, 128), :] = r_e[0, pl.ds(3 * i, 3), :]
    for j in range(2):
        at = row_of(1, 3, 0, 3, element(1, j, 1))
        dofs[pl.ds(at, 3, 32), :] = r_e[1, pl.ds(3 * j, 3), :]


def to_grid(dofs, outs):
    for comp in range(3):
        for x, i, a in owners(comp, 0):
            for y, j, b in owners(comp, 1):
                for k in range(2):
                    count = 3 + k * (comp != 2)
                    at = row_of(comp, a, b, 0, element(i, j, k))
                    outs[comp][x, y, pl.ds(3 * k, count), :] = dofs[pl.ds(at, count, 8), :]


def pack_shared(dofs, pack_x, pack_y, edges):
    for side in range(2):
        c = 3 * side
        for x, i, a in owners(0, 0):
            for j in range(2):
                at = row_of(0, a, 0, c, element(i, j, side))
                pack_x[side, x, pl.ds(3 * j, 3 + j), :] = dofs[pl.ds(at, 3 + j, 32), :]
        for x, i, a in owners(1, 0):
            for j in range(2):
                at = row_of(1, a, 0, c, element(i, j, side))
                pack_y[side, x, pl.ds(3 * j, 3), :] = dofs[pl.ds(at, 3, 32), :]
    for n, (first, second) in enumerate(SIGNS):
        p, q = first > 0, second > 0
        for i in range(2):
            at = row_of(0, 0, 3 * p, 3 * q, element(i, int(p), int(q)))
            edges[0, n, pl.ds(3 * i, 3), :] = dofs[pl.ds(at, 3, 128), :]
        for j in range(2):
            at = row_of(1, 3 * p, 0, 3 * q, element(int(p), j, int(q)))
            edges[1, n, pl.ds(3 * j, 3), :] = dofs[pl.ds(at, 3, 32), :]


def add_shared(outs, f_x, f_y, f_zx, f_zy, f_e):
    out_x, out_y, out_z = outs
    for side in range(2):
        at = 6 * side
        out_y[at] = out_y[at] + f_x[0][side]
        out_z[at] = out_z[at] + f_x[1][side]
        for x in range(6):
            out_x[x, at] = out_x[x, at] + f_y[0][side, x]
        for x in range(7):
            out_z[x, at] = out_z[x, at] + f_y[1][side, x]
        z = pl.ds(at, 1)
        for x in range(6):
            for y in range(7):
                out_x[x, y, z, :] = out_x[x, y, z, :] + f_zx[side, x, pl.ds(y, 1), :]
        for x in range(7):
            for y in range(6):
                out_y[x, y, z, :] = out_y[x, y, z, :] + f_zy[side, x, pl.ds(y, 1), :]
    for n, (first, second) in enumerate(SIGNS):
        p, q = 6 * (first > 0), 6 * (second > 0)
        for x in range(6):
            z = pl.ds(q, 1)
            out_x[x, p, z, :] = out_x[x, p, z, :] + f_e[0, n, pl.ds(x, 1), :]
        for y in range(6):
            z = pl.ds(q, 1)
            out_y[p, y, z, :] = out_y[p, y, z, :] + f_e[1, n, pl.ds(y, 1), :]
        out_z[p, q] = out_z[p, q] + f_e[2, n]


def kernel(
    sizes,
    vec_hbm,
    flip_hbm,
    rel_hbm,
    con_hbm,
    out_x,
    out_y,
    out_z,
    vec,
    flip,
    rel,
    con,
    flat,
    sign,
    mass,
    curl,
    dofs,
    temp,
    u_x,
    u_y,
    c_x,
    c_y,
    c_z,
    s_z,
    s_e,
    r_x,
    r_y,
    r_z,
    r_e,
    pack_x,
    pack_y,
    edges,
    f_xy,
    f_xz,
    f_yx,
    f_yz,
    f_zx,
    f_zy,
    f_e,
    load_sem,
    send_sem,
    recv_sem,
):
    me = [lax.axis_index(axis) for axis in AXES]

    def neighbour(*steps):
        return tuple(lax.rem(me[n] + steps[n] + sizes[n], sizes[n]) for n in range(3))

    loads = [
        pltpu.make_async_copy(source, target, load_sem.at[n])
        for n, (source, target) in enumerate(
            ((vec_hbm, vec), (flip_hbm, flip), (rel_hbm, rel), (con_hbm, con))
        )
    ]
    for copy in loads:
        copy.start()

    barrier = pltpu.get_barrier_semaphore()
    around = []
    for axis in range(3):
        for step in (-1, 1):
            around.append([step * (axis == n) for n in range(3)])
    for pair in EDGE_AXES:
        for first, second in SIGNS:
            around.append([first * (n == pair[0]) + second * (n == pair[1]) for n in range(3)])
    for steps in around:
        pl.semaphore_signal(barrier, inc=1, device_id=neighbour(*steps), device_id_type=MESH)

    copies = []

    def send(source, target, *steps):
        n = len(copies)
        copy = pltpu.make_async_remote_copy(
            src_ref=source,
            dst_ref=target,
            send_sem=send_sem.at[n],
            recv_sem=recv_sem.at[n],
            device_id=neighbour(*steps),
            device_id_type=MESH,
        )
        copy.start()
        copies.append(copy)

    loads[0].wait()
    for comp in range(2):
        for x in range(6):
            for y in range(6):
                s_z[comp, x, pl.ds(y, 1), :] = vec[comp, x, y, pl.ds(0, 1), :]
    for n in range(6):
        s_e[0, pl.ds(n, 1), :] = vec[0, n, 0, pl.ds(0, 1), :]
        s_e[1, pl.ds(n, 1), :] = vec[1, 0, n, pl.ds(0, 1), :]
    pl.semaphore_wait(barrier, len(around))
    send(vec.at[0, :, 0], r_y.at[0], 0, -1, 0)
    send(vec.at[2, :, 0], r_y.at[1], 0, -1, 0)
    send(vec.at[pl.ds(1, 2), 0], r_x, -1, 0, 0)
    send(s_z, r_z, 0, 0, -1)
    send(s_e.at[0], r_e.at[0], 0, -1, -1)
    send(s_e.at[1], r_e.at[1], -1, 0, -1)
    send(vec.at[2, 0, 0], r_e.at[2], -1, -1, 0)

    scatter_own(vec, dofs)
    for copy in loads[1:]:
        copy.wait()
    prepare(flip, rel, con, flat, sign, mass, curl)
    for copy in copies:
        copy.wait_recv()
    scatter_halo(dofs, r_x, r_y, r_z, r_e)
    compute(dofs, sign, mass, curl, temp, u_x, u_y, c_x, c_y, c_z)
    join_elements(dofs)
    outs = (out_x, out_y, out_z)
    to_grid(dofs, outs)
    pack_shared(dofs, pack_x, pack_y, edges)

    halo = len(copies)
    for side, step in enumerate((-1, 1)):
        at, other = 6 * side, 1 - side
        send(out_x.at[:, at], f_yx.at[other], 0, step, 0)
        send(out_z.at[:, at], f_yz.at[other], 0, step, 0)
        send(out_y.at[at], f_xy.at[other], step, 0, 0)
        send(out_z.at[at], f_xz.at[other], step, 0, 0)
        send(pack_x.at[side], f_zx.at[other], 0, 0, step)
        send(pack_y.at[side], f_zy.at[other], 0, 0, step)
    for n, (first, second) in enumerate(SIGNS):
        p, q = 6 * (first > 0), 6 * (second > 0)
        send(edges.at[0, n], f_e.at[0, 3 - n], 0, first, second)
        send(edges.at[1, n], f_e.at[1, 3 - n], first, 0, second)
        send(out_z.at[p, q], f_e.at[2, 3 - n], first, second, 0)
    for copy in copies[halo:]:
        copy.wait_recv()
    for copy in copies:
        copy.wait_send()
    add_shared(outs, (f_xy, f_xz), (f_yx, f_yz), f_zx, f_zy, f_e)


def on_device(sizes, vectors, orient_flip, reluctivity, conductivity):
    f32 = jnp.float32
    regs = lambda n: pltpu.VMEM((n, 8, LANES), f32)
    grid = ((6, 7, 7, LANES), (7, 6, 7, LANES), (7, 7, 6, LANES))
    return pl.pallas_call(
        lambda *refs: kernel(sizes, *refs),
        out_shape=[jax.ShapeDtypeStruct(shape, f32) for shape in grid],
        in_specs=[pl.BlockSpec(memory_space=pl.ANY)] * 4,
        out_specs=[pl.BlockSpec(memory_space=pltpu.VMEM)] * 3,
        scratch_shapes=[
            pltpu.VMEM((3, 6, 6, 6, LANES), f32),
            pltpu.VMEM(orient_flip.shape, jnp.int32),
            pltpu.VMEM(reluctivity.shape, f32),
            pltpu.VMEM(conductivity.shape, f32),
            pltpu.VMEM((8, 512), f32),
            regs(DOFS),
            regs(QPTS),
            regs(QPTS),
            pltpu.VMEM((8 * DOFS, LANES), f32),
            regs(QPTS),
            regs(QPTS),
            regs(QPTS),
            regs(QPTS),
            regs(QPTS),
            regs(QPTS),
            pltpu.VMEM((2, 6, 6, LANES), f32),
            pltpu.VMEM((2, 6, LANES), f32),
            pltpu.VMEM((2, 6, 6, LANES), f32),
            pltpu.VMEM((2, 6, 6, LANES), f32),
            pltpu.VMEM((2, 6, 6, LANES), f32),
            pltpu.VMEM((3, 6, LANES), f32),
            pltpu.VMEM((2, 6, 7, LANES), f32),
            pltpu.VMEM((2, 7, 6, LANES), f32),
            pltpu.VMEM((2, 4, 6, LANES), f32),
            pltpu.VMEM((2, 6, 7, LANES), f32),
            pltpu.VMEM((2, 7, 6, LANES), f32),
            pltpu.VMEM((2, 6, 7, LANES), f32),
            pltpu.VMEM((2, 7, 6, LANES), f32),
            pltpu.VMEM((2, 6, 7, LANES), f32),
            pltpu.VMEM((2, 7, 6, LANES), f32),
            pltpu.VMEM((3, 4, 6, LANES), f32),
            pltpu.SemaphoreType.DMA((4,)),
            pltpu.SemaphoreType.DMA((31,)),
            pltpu.SemaphoreType.DMA((31,)),
        ],
        compiler_params=pltpu.CompilerParams(collective_id=0, has_side_effects=True),
        name="curlcurl",
    )(vectors, orient_flip, reluctivity, conductivity)


def solution(mesh):
    sizes = tuple(mesh.shape[axis] for axis in AXES)
    return jax.shard_map(
        lambda *args: tuple(on_device(sizes, *args)),
        mesh=mesh,
        in_specs=(
            P(None, "gx", "gy", "gz", None),
            P("gx", "gy", "gz"),
            P("gx", "gy", "gz"),
            P("gx", "gy", "gz"),
        ),
        out_specs=(P("gx", "gy", "gz", None), P("gx", "gy", "gz", None), P("gx", "gy", "gz", None)),
        check_vma=False,
    )
```

```python
import jax
import jax.numpy as jnp
import numpy as np
from jax import lax
from jax.experimental import pallas as pl
from jax.experimental.pallas import tpu as pltpu
from jax.sharding import PartitionSpec as P

MESH = pl.DeviceIdType.MESH
AXES = ("gx", "gy", "gz")
LANES = 128
DOFS = 144
QPTS = 64
BASE = (0, 48, 96)
STRIDE = ((16, 4, 1), (12, 4, 1), (12, 3, 1))
EDGE_AXES = ((1, 2), (0, 2), (0, 1))
SIGNS = ((-1, -1), (-1, 1), (1, -1), (1, 1))


def lagrange(points_at, evaluate_at):
    amount = len(points_at)
    values = np.ones((len(evaluate_at), amount))
    slopes = np.zeros((len(evaluate_at), amount))
    for which in range(amount):
        for column in range(amount):
            if column != which:
                factor = (evaluate_at - points_at[column]) / (points_at[which] - points_at[column])
                slopes[:, which] = slopes[:, which] * factor + values[:, which] / (
                    points_at[which] - points_at[column]
                )
                values[:, which] = values[:, which] * factor
    return (values, slopes)


def basis_tables():
    lobatto = np.array([0.0, (1 - 5 ** (-0.5)) / 2, (1 + 5 ** (-0.5)) / 2, 1.0])
    gauss_open = np.array([(1 - 0.6**0.5) / 2, 0.5, (1 + 0.6**0.5) / 2])
    inner_pt = (3.0 / 7 - 2.0 / 7 * (6.0 / 5) ** 0.5) ** 0.5
    outer_pt = (3.0 / 7 + 2.0 / 7 * (6.0 / 5) ** 0.5) ** 0.5
    inner_wt = (18 + 30**0.5) / 36
    outer_wt = (18 - 30**0.5) / 36
    quad_points = (1 + np.array([-outer_pt, -inner_pt, inner_pt, outer_pt])) / 2
    quad_weight = np.array([outer_wt, inner_wt, inner_wt, outer_wt]) / 2
    closed, slopes = lagrange(lobatto, quad_points)
    opened, unused_slopes = lagrange(gauss_open, quad_points)
    return (closed, slopes, opened, quad_weight)


CLOSED, SLOPES, OPENED, WEIGHT = basis_tables()
DERIV = SLOPES @ np.linalg.inv(CLOSED)


def apply(table, given, parity):
    rows, columns = table.shape
    half = columns // 2
    sums = [given[c] + given[columns - 1 - c] for c in range(half)]
    diffs = [given[c] - given[columns - 1 - c] for c in range(half)]
    result = [None] * rows
    for q in range((rows + 1) // 2):
        even = None
        for c in range(half):
            term = sums[c] * float((table[q, c] + table[q, columns - 1 - c]) / 2)
            even = term if even is None else even + term
        if columns % 2:
            even = even + given[half] * float(table[q, half])
        if 2 * q + 1 == rows:
            result[q] = even
            continue
        odd = None
        for c in range(half):
            term = diffs[c] * float((table[q, c] - table[q, columns - 1 - c]) / 2)
            odd = term if odd is None else odd + term
        result[q] = even + odd
        result[rows - 1 - q] = even - odd if parity > 0 else odd - even
    return result


def along_rows(table, plane, parity=1):
    columns = [apply(table, [row[c] for row in plane], parity) for c in range(len(plane[0]))]
    return [[column[q] for column in columns] for q in range(table.shape[0])]


def along_columns(table, plane, parity=1):
    return [apply(table, row, parity) for row in plane]


def combine(op, *planes):
    return [[op(*entries) for entries in zip(*rows)] for rows in zip(*planes)]


def plus(p, q):
    return combine(lambda s, t: s + t, p, q)


def minus(p, q):
    return combine(lambda s, t: s - t, p, q)


def times(p, q):
    return combine(lambda s, t: s * t, p, q)


def dof(comp, a, b, c):
    s = STRIDE[comp]
    return BASE[comp] + a * s[0] + b * s[1] + c * s[2]


def row_of(comp, a, b, c, element=0):
    return 8 * dof(comp, a, b, c) + element


def element(i, j, k):
    return 4 * k + 2 * i + j


def places(comp, axis):
    if comp == axis:
        return [(g, g // 3, g % 3) for g in range(6)]
    return [(g, 0, g) for g in range(4)] + [(g, 1, g - 3) for g in range(3, 7)]


def owners(comp, axis):
    last = 6 if comp == axis else 7
    return [(g, min(g // 3, 1), g - 3 * min(g // 3, 1)) for g in range(last)]


def prepare(flip, rel, con, flat, sign, mass, curl):
    for k in range(2):
        for i in range(2):
            at = pl.ds(4 * k + 2 * i, 2)
            flat[at, 0:DOFS] = 1.0 - 2.0 * flip[i][:, DOFS * k : DOFS * (k + 1)].astype(jnp.float32)
            flat[at, 256 : 256 + QPTS] = rel[i][:, QPTS * k : QPTS * (k + 1)]
            flat[at, 384 : 384 + QPTS] = con[i][:, QPTS * k : QPTS * (k + 1)]
    whole = flat[:, 0:DOFS]
    for d in range(DOFS):
        sign[d] = jnp.broadcast_to(whole[:, d : d + 1], (8, LANES))
    rel_all = flat[:, 256 : 256 + QPTS]
    con_all = flat[:, 384 : 384 + QPTS]
    for q in range(QPTS):
        weight = float(WEIGHT[q // 16] * WEIGHT[q // 4 % 4] * WEIGHT[q % 4])
        curl[q] = jnp.broadcast_to(rel_all[:, q : q + 1], (8, LANES)) * weight
        mass[q] = jnp.broadcast_to(con_all[:, q : q + 1], (8, LANES)) * weight


def quad(x, y, z):
    return 16 * x + 4 * y + z


def planes(ref, at):
    return [[ref[at(p, q)] for q in range(4)] for p in range(4)]


def put(ref, at, plane):
    for p, row in enumerate(plane):
        for q, value in enumerate(row):
            ref[at(p, q)] = value


def load_plane(dofs, sign, rows):
    return [
        [dofs[pl.ds(pl.multiple_of(8 * d, 8), 8), :] * sign[d] for d in row] for row in rows
    ]


def store_plane(dofs, sign, rows, plane):
    for row, values in zip(rows, plane):
        for d, value in zip(row, values):
            dofs[pl.ds(pl.multiple_of(8 * d, 8), 8), :] = value * sign[d]


def rows_fixed_b(comp, b):
    return [[dof(comp, a, b, c) for c in range(4 - (comp == 2))] for a in range(4 - (comp == 0))]


def rows_fixed_a(comp, a):
    return [[dof(comp, a, b, c) for c in range(4)] for b in range(3)]


def forward_y(dofs, sign, temp, u_y, c_x, c_z):
    @pl.loop(0, 4)
    def _(a):
        values = along_rows(OPENED, load_plane(dofs, sign, rows_fixed_a(1, a)))
        put(temp, lambda y, z: quad(a, y, z), along_columns(CLOSED, values))

    @pl.loop(0, 4)
    def _(y):
        at = lambda x, z: quad(x, y, z)
        u = along_rows(CLOSED, planes(temp, at))
        put(u_y, at, u)
        put(c_z, at, along_rows(DERIV, u, -1))
        put(c_x, at, along_columns(-DERIV, u, -1))


def start_x(dofs, sign, temp, b):
    values = along_rows(OPENED, load_plane(dofs, sign, rows_fixed_b(0, b)))
    put(temp, lambda x, z: quad(x, b, z), along_columns(CLOSED, values))


def start_z(dofs, sign, temp, b):
    values = along_columns(OPENED, load_plane(dofs, sign, rows_fixed_b(2, b)))
    put(temp, lambda x, z: quad(x, b, z), along_rows(CLOSED, values))


def forward_x(temp, curl, u_x, c_y, c_z):
    @pl.loop(0, 4)
    def _(x):
        at = lambda y, z: quad(x, y, z)
        u = along_rows(CLOSED, planes(temp, at))
        put(u_x, at, u)
        w_z = minus(planes(c_z, at), along_rows(DERIV, u, -1))
        put(c_z, at, times(planes(curl, at), w_z))
        put(c_y, at, along_columns(DERIV, u, -1))


def turn_z(temp, mass, curl, c_x, c_y):
    @pl.loop(0, 4)
    def _(z):
        at = lambda x, y: quad(x, y, z)
        u = along_columns(CLOSED, planes(temp, at))
        scale = planes(curl, at)
        w_y = times(scale, minus(planes(c_y, at), along_rows(DERIV, u, -1)))
        w_x = times(scale, plus(planes(c_x, at), along_columns(DERIV, u, -1)))
        put(c_y, at, w_y)
        put(c_x, at, w_x)
        v = times(planes(mass, at), u)
        v = plus(v, along_columns(DERIV.T, w_x, -1))
        v = minus(v, along_rows(DERIV.T, w_y, -1))
        put(temp, at, along_columns(CLOSED.T, v))


def finish_z(dofs, sign, temp):
    @pl.loop(0, 4)
    def _(b):
        values = along_rows(CLOSED.T, planes(temp, lambda x, z: quad(x, b, z)))
        store_plane(dofs, sign, rows_fixed_b(2, b), along_columns(OPENED.T, values))


def backward_x(dofs, sign, mass, temp, u_x, c_y, c_z):
    @pl.loop(0, 4)
    def _(x):
        at = lambda y, z: quad(x, y, z)
        v = times(planes(mass, at), planes(u_x, at))
        v = plus(v, along_columns(DERIV.T, planes(c_y, at), -1))
        v = minus(v, along_rows(DERIV.T, planes(c_z, at), -1))
        put(temp, at, along_rows(CLOSED.T, v))

    @pl.loop(0, 4)
    def _(b):
        values = along_columns(CLOSED.T, planes(temp, lambda x, z: quad(x, b, z)))
        store_plane(dofs, sign, rows_fixed_b(0, b), along_rows(OPENED.T, values))


def backward_y(dofs, sign, mass, temp, u_y, c_x, c_z):
    @pl.loop(0, 4)
    def _(y):
        at = lambda x, z: quad(x, y, z)
        v = times(planes(mass, at), planes(u_y, at))
        v = plus(v, along_rows(DERIV.T, planes(c_z, at), -1))
        v = minus(v, along_columns(DERIV.T, planes(c_x, at), -1))
        put(temp, at, along_rows(CLOSED.T, v))

    @pl.loop(0, 4)
    def _(a):
        values = along_columns(CLOSED.T, planes(temp, lambda y, z: quad(a, y, z)))
        store_plane(dofs, sign, rows_fixed_a(1, a), along_rows(OPENED.T, values))


def join_elements(dofs, comp):
    rows = lax.broadcasted_iota(jnp.int32, (8, LANES), 0)
    for axis, step in ((0, 2), (1, 1), (2, 4)):
        if comp == axis:
            continue
        upper = (rows // step) % 2 == 1
        sizes = [3 if comp == other else 4 for other in range(3)]
        sizes[axis] = 1
        for a in range(sizes[0]):
            for b in range(sizes[1]):
                for c in range(sizes[2]):
                    high = [a, b, c]
                    high[axis] = 3
                    to = pl.ds(row_of(comp, a, b, c), 8)
                    moved = pltpu.roll(dofs[pl.ds(row_of(comp, *high), 8), :], step, 0)
                    dofs[to, :] = dofs[to, :] + jnp.where(upper, moved, 0.0)


def scatter_own(vec, dofs):
    for comp in range(3):
        for x, i, a in places(comp, 0):
            for y, j, b in places(comp, 1):
                if x == 6 or y == 6:
                    continue
                for k in range(2):
                    count = 4 if comp != 2 and k == 0 else 3
                    at = row_of(comp, a, b, 0, element(i, j, k))
                    dofs[pl.ds(at, count, 8), :] = vec[comp, x, y, pl.ds(3 * k, count), :]


def scatter_line(dofs, comp, i, a, j, b, source):
    for k in range(2):
        count = 4 if comp != 2 and k == 0 else 3
        at = row_of(comp, a, b, 0, element(i, j, k))
        dofs[pl.ds(at, count, 8), :] = source(pl.ds(3 * k, count))


def scatter_xz_halo(dofs, r_x, r_z, r_e):
    for comp in (1, 2):
        for y, j, b in places(comp, 1):
            if y < 6:
                scatter_line(dofs, comp, 1, 3, j, b, lambda z: r_x[comp - 1, y, z, :])
    for x, i, a in places(0, 0):
        for j in range(2):
            count = 4 - j
            at = row_of(0, a, 0, 3, element(i, j, 1))
            dofs[pl.ds(at, count, 32), :] = r_z[0, x, pl.ds(3 * j, count), :]
    for x, i, a in places(1, 0):
        if x < 6:
            for j in range(2):
                at = row_of(1, a, 0, 3, element(i, j, 1))
                dofs[pl.ds(at, 3, 32), :] = r_z[1, x, pl.ds(3 * j, 3), :]
    for j in range(2):
        at = row_of(1, 3, 0, 3, element(1, j, 1))
        dofs[pl.ds(at, 3, 32), :] = r_e[1, pl.ds(3 * j, 3), :]


def scatter_y_halo(dofs, r_y, r_e):
    for comp in (0, 2):
        for x, i, a in places(comp, 0):
            if x < 6:
                scatter_line(dofs, comp, i, a, 1, 3, lambda z: r_y[comp // 2, x, z, :])
    scatter_line(dofs, 2, 1, 3, 1, 3, lambda z: r_e[2, z, :])
    for i in range(2):
        at = row_of(0, 0, 3, 3, element(i, 1, 1))
        dofs[pl.ds(at, 3, 128), :] = r_e[0, pl.ds(3 * i, 3), :]


def runs(comp, axis, fixed):
    local = [None if g is None else owners(comp, n)[g][1:] for n, g in enumerate(fixed)]
    result = []
    for half in range(2):
        count = 3 + half * (comp != axis)
        at = [(half, 0) if entry is None else entry for entry in local]
        (i, a), (j, b), (k, c) = at
        row = row_of(comp, a, b, c, element(i, j, k))
        result.append((pl.ds(3 * half, count), pl.ds(row, count, 8 * STRIDE[comp][axis])))
    return result


def owned(comp, axis):
    return range(6 if comp == axis else 7)


def to_grid(dofs, comp, out, line):
    other = 3 - line
    for x in owned(comp, 0):
        for q in owned(comp, other):
            fixed = [x, None, None]
            fixed[other] = q
            for grid, rows in runs(comp, line, fixed):
                out[x, q, grid, :] = dofs[rows, :]


def pack_face(dofs, comp, axis, line, pack):
    third = 3 - axis - line
    for side in range(2):
        for p in owned(comp, third):
            fixed = [None] * 3
            fixed[axis] = 6 * side
            fixed[third] = p
            for grid, rows in runs(comp, line, fixed):
                pack[side, p, grid, :] = dofs[rows, :]


def add_face(dofs, comp, axis, line, given):
    third = 3 - axis - line
    for side in range(2):
        for p in owned(comp, third):
            fixed = [None] * 3
            fixed[axis] = 6 * side
            fixed[third] = p
            for grid, rows in runs(comp, line, fixed):
                dofs[rows, :] = dofs[rows, :] + given[side, p, grid, :]


def edge_runs(comp, n):
    fixed = [None] * 3
    for axis, sign in zip(EDGE_AXES[comp], SIGNS[n]):
        fixed[axis] = 6 * (sign > 0)
    return runs(comp, comp, fixed)


def pack_edges(dofs, comp, edges):
    for n in range(4):
        for grid, rows in edge_runs(comp, n):
            edges[comp, n, grid, :] = dofs[rows, :]


def add_edges(dofs, comp, given):
    for n in range(4):
        for grid, rows in edge_runs(comp, n):
            dofs[rows, :] = dofs[rows, :] + given[comp, n, grid, :]


def kernel(
    sizes,
    vec_hbm,
    flip_hbm,
    rel_hbm,
    con_hbm,
    out_x,
    out_y,
    out_z,
    vec,
    flip,
    rel,
    con,
    flat,
    sign,
    mass,
    curl,
    dofs,
    temp,
    u_x,
    u_y,
    c_x,
    c_y,
    c_z,
    s_z,
    s_e,
    r_x,
    r_y,
    r_z,
    r_e,
    t_x,
    t_z,
    p_xy,
    p_xz,
    p_yx,
    p_yz,
    p_zx,
    p_zy,
    p_e,
    f_xy,
    f_xz,
    f_yx,
    f_yz,
    f_zx,
    f_zy,
    f_e,
    load_sem,
    send_sem,
    recv_sem,
):
    me = [lax.axis_index(axis) for axis in AXES]

    def neighbour(*steps):
        return tuple(lax.rem(me[n] + steps[n] + sizes[n], sizes[n]) for n in range(3))

    loads = [
        pltpu.make_async_copy(source, target, load_sem.at[n])
        for n, (source, target) in enumerate(
            ((vec_hbm, vec), (flip_hbm, flip), (rel_hbm, rel), (con_hbm, con))
        )
    ]
    for copy in loads:
        copy.start()

    barrier = pltpu.get_barrier_semaphore()
    around = []
    for axis in range(3):
        for step in (-1, 1):
            around.append([step * (axis == n) for n in range(3)])
    for pair in EDGE_AXES:
        for first, second in SIGNS:
            around.append([first * (n == pair[0]) + second * (n == pair[1]) for n in range(3)])
    for steps in around:
        pl.semaphore_signal(barrier, inc=1, device_id=neighbour(*steps), device_id_type=MESH)

    copies = []

    def send(source, target, *steps):
        n = len(copies)
        copy = pltpu.make_async_remote_copy(
            src_ref=source,
            dst_ref=target,
            send_sem=send_sem.at[n],
            recv_sem=recv_sem.at[n],
            device_id=neighbour(*steps),
            device_id_type=MESH,
        )
        copy.start()
        copies.append(copy)
        return copy

    def send_faces(axis, pack, target):
        faces = []
        for side in range(2):
            steps = [(2 * side - 1) * (axis == n) for n in range(3)]
            faces.append(send(pack.at[side], target.at[1 - side], *steps))
        return faces

    def send_edges(comp):
        sent = []
        for n, pair in enumerate(SIGNS):
            steps = [0, 0, 0]
            for axis, step in zip(EDGE_AXES[comp], pair):
                steps[axis] = step
            sent.append(send(p_e.at[comp, n], f_e.at[comp, 3 - n], *steps))
        return sent

    def receive(arriving):
        for copy in arriving:
            copy.wait_recv()

    loads[0].wait()
    for comp in range(2):
        for x in range(6):
            for y in range(6):
                s_z[comp, x, pl.ds(y, 1), :] = vec[comp, x, y, pl.ds(0, 1), :]
    for n in range(6):
        s_e[0, pl.ds(n, 1), :] = vec[0, n, 0, pl.ds(0, 1), :]
        s_e[1, pl.ds(n, 1), :] = vec[1, 0, n, pl.ds(0, 1), :]
    pl.semaphore_wait(barrier, len(around))
    y_halo = [
        send(vec.at[0, :, 0], r_y.at[0], 0, -1, 0),
        send(vec.at[2, :, 0], r_y.at[1], 0, -1, 0),
    ]
    xz_halo = [
        send(vec.at[pl.ds(1, 2), 0], r_x, -1, 0, 0),
        send(s_z, r_z, 0, 0, -1),
        send(s_e.at[1], r_e.at[1], -1, 0, -1),
    ]
    y_halo += [
        send(s_e.at[0], r_e.at[0], 0, -1, -1),
        send(vec.at[2, 0, 0], r_e.at[2], -1, -1, 0),
    ]

    scatter_own(vec, dofs)
    for copy in loads[1:]:
        copy.wait()
    prepare(flip, rel, con, flat, sign, mass, curl)
    receive(xz_halo)
    scatter_xz_halo(dofs, r_x, r_z, r_e)
    forward_y(dofs, sign, temp, u_y, c_x, c_z)

    @pl.loop(0, 3)
    def _(b):
        start_x(dofs, sign, t_x, b)
        start_z(dofs, sign, t_z, b)

    receive(y_halo)
    scatter_y_halo(dofs, r_y, r_e)
    start_x(dofs, sign, t_x, 3)
    start_z(dofs, sign, t_z, 3)
    forward_x(t_x, curl, u_x, c_y, c_z)
    turn_z(t_z, mass, curl, c_x, c_y)
    finish_z(dofs, sign, t_z)
    join_elements(dofs, 2)
    pack_face(dofs, 2, 1, 2, p_yz)
    faces_yz = send_faces(1, p_yz, f_yz)
    pack_edges(dofs, 2, p_e)
    edges_z = send_edges(2)
    pack_face(dofs, 2, 0, 1, p_xz)
    faces_xz = send_faces(0, p_xz, f_xz)

    backward_x(dofs, sign, mass, t_x, u_x, c_y, c_z)
    join_elements(dofs, 0)
    pack_face(dofs, 0, 1, 2, p_yx)
    faces_yx = send_faces(1, p_yx, f_yx)
    pack_edges(dofs, 0, p_e)
    edges_x = send_edges(0)
    pack_face(dofs, 0, 2, 1, p_zx)
    faces_zx = send_faces(2, p_zx, f_zx)

    backward_y(dofs, sign, mass, temp, u_y, c_x, c_z)
    join_elements(dofs, 1)
    pack_face(dofs, 1, 0, 2, p_xy)
    faces_xy = send_faces(0, p_xy, f_xy)
    pack_edges(dofs, 1, p_e)
    edges_y = send_edges(1)
    pack_face(dofs, 1, 2, 1, p_zy)
    faces_zy = send_faces(2, p_zy, f_zy)

    receive(faces_zx)
    add_face(dofs, 0, 2, 1, f_zx)
    to_grid(dofs, 0, out_x, 2)
    receive(faces_yz + edges_z)
    add_face(dofs, 2, 1, 2, f_yz)
    add_edges(dofs, 2, f_e)
    to_grid(dofs, 2, out_z, 1)
    receive(faces_xz)
    for side in range(2):
        out_z[6 * side] = out_z[6 * side] + f_xz[side]
    receive(faces_zy + edges_y)
    add_face(dofs, 1, 2, 1, f_zy)
    add_edges(dofs, 1, f_e)
    to_grid(dofs, 1, out_y, 2)
    receive(faces_xy)
    for side in range(2):
        out_y[6 * side] = out_y[6 * side] + f_xy[side]
    receive(edges_x)
    for n, pair in enumerate(SIGNS):
        y, z = 6 * (pair[0] > 0), 6 * (pair[1] > 0)
        for x in range(6):
            at = pl.ds(z, 1)
            out_x[x, y, at, :] = out_x[x, y, at, :] + f_e[0, n, pl.ds(x, 1), :]
    receive(faces_yx)
    for side in range(2):
        for x in range(6):
            out_x[x, 6 * side] = out_x[x, 6 * side] + f_yx[side, x]
    for copy in copies:
        copy.wait_send()


def put_out(in_x, in_y, in_z, out_x, out_y, out_z, sem):
    pairs = ((in_x, out_x), (in_y, out_y), (in_z, out_z))
    copies = [pltpu.make_async_copy(*pair, sem.at[n]) for n, pair in enumerate(pairs)]
    for copy in copies:
        copy.start()
    for copy in copies:
        copy.wait()


def on_device(sizes, vectors, orient_flip, reluctivity, conductivity):
    f32 = jnp.float32
    regs = lambda n: pltpu.VMEM((n, 8, LANES), f32)
    grid = ((6, 7, 7, LANES), (7, 6, 7, LANES), (7, 6, 7, LANES))
    faces = [
        pltpu.VMEM(shape, f32)
        for shape in (
            (2, 6, 7, LANES),
            (2, 6, 7, LANES),
            (2, 6, 7, LANES),
            (2, 7, 6, LANES),
            (2, 6, 7, LANES),
            (2, 7, 6, LANES),
            (3, 4, 6, LANES),
        )
    ]
    results = pl.pallas_call(
        lambda *refs: kernel(sizes, *refs),
        out_shape=[pltpu.VMEM(shape, f32) for shape in grid],
        in_specs=[pl.BlockSpec(memory_space=pl.ANY)] * 4,
        out_specs=[pl.BlockSpec(memory_space=pltpu.VMEM)] * 3,
        scratch_shapes=[
            pltpu.VMEM((3, 6, 6, 6, LANES), f32),
            pltpu.VMEM(orient_flip.shape, jnp.int32),
            pltpu.VMEM(reluctivity.shape, f32),
            pltpu.VMEM(conductivity.shape, f32),
            pltpu.VMEM((8, 512), f32),
            regs(DOFS),
            regs(QPTS),
            regs(QPTS),
            pltpu.VMEM((8 * DOFS, LANES), f32),
            regs(QPTS),
            regs(QPTS),
            regs(QPTS),
            regs(QPTS),
            regs(QPTS),
            regs(QPTS),
            pltpu.VMEM((2, 6, 6, LANES), f32),
            pltpu.VMEM((2, 6, LANES), f32),
            pltpu.VMEM((2, 6, 6, LANES), f32),
            pltpu.VMEM((2, 6, 6, LANES), f32),
            pltpu.VMEM((2, 6, 6, LANES), f32),
            pltpu.VMEM((3, 6, LANES), f32),
            regs(QPTS),
            regs(QPTS),
            *faces,
            *faces,
            pltpu.SemaphoreType.DMA((4,)),
            pltpu.SemaphoreType.DMA((31,)),
            pltpu.SemaphoreType.DMA((31,)),
        ],
        compiler_params=pltpu.CompilerParams(collective_id=0, has_side_effects=True),
        name="curlcurl",
    )(vectors, orient_flip, reluctivity, conductivity)
    results = [pltpu.with_memory_space_constraint(result, pltpu.VMEM) for result in results]
    out_x, out_y, out_z = pl.pallas_call(
        put_out,
        out_shape=[jax.ShapeDtypeStruct(shape, f32) for shape in grid],
        in_specs=[pl.BlockSpec(memory_space=pltpu.VMEM)] * 3,
        out_specs=[pl.BlockSpec(memory_space=pl.ANY)] * 3,
        scratch_shapes=[pltpu.SemaphoreType.DMA((3,))],
        name="putout",
    )(*results)
    return (out_x, out_y, jnp.swapaxes(out_z, 1, 2))


def solution(mesh):
    sizes = tuple(mesh.shape[axis] for axis in AXES)
    return jax.shard_map(
        lambda *args: on_device(sizes, *args),
        mesh=mesh,
        in_specs=(
            P(None, "gx", "gy", "gz", None),
            P("gx", "gy", "gz"),
            P("gx", "gy", "gz"),
            P("gx", "gy", "gz"),
        ),
        out_specs=(P("gx", "gy", "gz", None), P("gx", "gy", "gz", None), P("gx", "gy", "gz", None)),
        check_vma=False,
    )
```

```python
import jax
import jax.numpy as jnp
import numpy as np
from jax import lax
from jax.experimental import pallas as pl
from jax.experimental.pallas import tpu as pltpu
from jax.sharding import PartitionSpec as P

MESH = pl.DeviceIdType.MESH
AXES = ("gx", "gy", "gz")
LANES = 128
DOFS = 144
QPTS = 64
BASE = (0, 48, 96)
STRIDE = ((16, 4, 1), (12, 4, 1), (12, 3, 1))
EDGE_AXES = ((1, 2), (0, 2), (0, 1))
SIGNS = ((-1, -1), (-1, 1), (1, -1), (1, 1))


def lagrange(points_at, evaluate_at):
    amount = len(points_at)
    values = np.ones((len(evaluate_at), amount))
    slopes = np.zeros((len(evaluate_at), amount))
    for which in range(amount):
        for column in range(amount):
            if column != which:
                factor = (evaluate_at - points_at[column]) / (points_at[which] - points_at[column])
                slopes[:, which] = slopes[:, which] * factor + values[:, which] / (
                    points_at[which] - points_at[column]
                )
                values[:, which] = values[:, which] * factor
    return (values, slopes)


def basis_tables():
    lobatto = np.array([0.0, (1 - 5 ** (-0.5)) / 2, (1 + 5 ** (-0.5)) / 2, 1.0])
    gauss_open = np.array([(1 - 0.6**0.5) / 2, 0.5, (1 + 0.6**0.5) / 2])
    inner_pt = (3.0 / 7 - 2.0 / 7 * (6.0 / 5) ** 0.5) ** 0.5
    outer_pt = (3.0 / 7 + 2.0 / 7 * (6.0 / 5) ** 0.5) ** 0.5
    inner_wt = (18 + 30**0.5) / 36
    outer_wt = (18 - 30**0.5) / 36
    quad_points = (1 + np.array([-outer_pt, -inner_pt, inner_pt, outer_pt])) / 2
    quad_weight = np.array([outer_wt, inner_wt, inner_wt, outer_wt]) / 2
    closed, slopes = lagrange(lobatto, quad_points)
    opened, unused_slopes = lagrange(gauss_open, quad_points)
    return (closed, slopes, opened, quad_weight)


CLOSED, SLOPES, OPENED, WEIGHT = basis_tables()
DERIV = SLOPES @ np.linalg.inv(CLOSED)


def apply(table, given, parity):
    rows, columns = table.shape
    half = columns // 2
    sums = [given[c] + given[columns - 1 - c] for c in range(half)]
    diffs = [given[c] - given[columns - 1 - c] for c in range(half)]
    result = [None] * rows
    for q in range((rows + 1) // 2):
        even = None
        for c in range(half):
            term = sums[c] * float((table[q, c] + table[q, columns - 1 - c]) / 2)
            even = term if even is None else even + term
        if columns % 2:
            even = even + given[half] * float(table[q, half])
        if 2 * q + 1 == rows:
            result[q] = even
            continue
        odd = None
        for c in range(half):
            term = diffs[c] * float((table[q, c] - table[q, columns - 1 - c]) / 2)
            odd = term if odd is None else odd + term
        result[q] = even + odd
        result[rows - 1 - q] = even - odd if parity > 0 else odd - even
    return result


def along_rows(table, plane, parity=1):
    columns = [apply(table, [row[c] for row in plane], parity) for c in range(len(plane[0]))]
    return [[column[q] for column in columns] for q in range(table.shape[0])]


def along_columns(table, plane, parity=1):
    return [apply(table, row, parity) for row in plane]


def combine(op, *planes):
    return [[op(*entries) for entries in zip(*rows)] for rows in zip(*planes)]


def plus(p, q):
    return combine(lambda s, t: s + t, p, q)


def minus(p, q):
    return combine(lambda s, t: s - t, p, q)


def times(p, q):
    return combine(lambda s, t: s * t, p, q)


def dof(comp, a, b, c):
    s = STRIDE[comp]
    return BASE[comp] + a * s[0] + b * s[1] + c * s[2]


def row_of(comp, a, b, c, element=0):
    return 8 * dof(comp, a, b, c) + element


def element(i, j, k):
    return 4 * k + 2 * i + j


def places(comp, axis):
    if comp == axis:
        return [(g, g // 3, g % 3) for g in range(6)]
    return [(g, 0, g) for g in range(4)] + [(g, 1, g - 3) for g in range(3, 7)]


def owners(comp, axis):
    last = 6 if comp == axis else 7
    return [(g, min(g // 3, 1), g - 3 * min(g // 3, 1)) for g in range(last)]


def prepare(flip, rel, con, flat, sign, mass, curl):
    for k in range(2):
        for i in range(2):
            at = pl.ds(4 * k + 2 * i, 2)
            flat[at, 0:DOFS] = 1.0 - 2.0 * flip[i][:, DOFS * k : DOFS * (k + 1)].astype(jnp.float32)
            flat[at, 256 : 256 + QPTS] = rel[i][:, QPTS * k : QPTS * (k + 1)]
            flat[at, 384 : 384 + QPTS] = con[i][:, QPTS * k : QPTS * (k + 1)]
    whole = flat[:, 0:DOFS]
    for d in range(DOFS):
        sign[d] = jnp.broadcast_to(whole[:, d : d + 1], (8, LANES))
    rel_all = flat[:, 256 : 256 + QPTS]
    con_all = flat[:, 384 : 384 + QPTS]
    for q in range(QPTS):
        weight = float(WEIGHT[q // 16] * WEIGHT[q // 4 % 4] * WEIGHT[q % 4])
        curl[q] = jnp.broadcast_to(rel_all[:, q : q + 1], (8, LANES)) * weight
        mass[q] = jnp.broadcast_to(con_all[:, q : q + 1], (8, LANES)) * weight


def quad(x, y, z):
    return 16 * x + 4 * y + z


def planes(ref, at):
    return [[ref[at(p, q)] for q in range(4)] for p in range(4)]


def put(ref, at, plane):
    for p, row in enumerate(plane):
        for q, value in enumerate(row):
            ref[at(p, q)] = value


def load_plane(dofs, sign, rows):
    return [
        [dofs[pl.ds(pl.multiple_of(8 * d, 8), 8), :] * sign[d] for d in row] for row in rows
    ]


def store_plane(dofs, sign, rows, plane):
    for row, values in zip(rows, plane):
        for d, value in zip(row, values):
            dofs[pl.ds(pl.multiple_of(8 * d, 8), 8), :] = value * sign[d]


def rows_fixed_b(comp, b):
    return [[dof(comp, a, b, c) for c in range(4 - (comp == 2))] for a in range(4 - (comp == 0))]


def rows_fixed_a(comp, a):
    return [[dof(comp, a, b, c) for c in range(4)] for b in range(3)]


def forward_y(dofs, sign, temp, u_y, c_x, c_z):
    @pl.loop(0, 4)
    def _(a):
        values = along_rows(OPENED, load_plane(dofs, sign, rows_fixed_a(1, a)))
        put(temp, lambda y, z: quad(a, y, z), along_columns(CLOSED, values))

    @pl.loop(0, 4)
    def _(y):
        at = lambda x, z: quad(x, y, z)
        u = along_rows(CLOSED, planes(temp, at))
        put(u_y, at, u)
        put(c_z, at, along_rows(DERIV, u, -1))
        put(c_x, at, along_columns(-DERIV, u, -1))


def start_x(dofs, sign, temp, b):
    values = along_rows(OPENED, load_plane(dofs, sign, rows_fixed_b(0, b)))
    put(temp, lambda x, z: quad(x, b, z), along_columns(CLOSED, values))


def start_z(dofs, sign, temp, b):
    values = along_columns(OPENED, load_plane(dofs, sign, rows_fixed_b(2, b)))
    put(temp, lambda x, z: quad(x, b, z), along_rows(CLOSED, values))


def forward_x(temp, curl, u_x, c_y, c_z):
    @pl.loop(0, 4)
    def _(x):
        at = lambda y, z: quad(x, y, z)
        u = along_rows(CLOSED, planes(temp, at))
        put(u_x, at, u)
        w_z = minus(planes(c_z, at), along_rows(DERIV, u, -1))
        put(c_z, at, times(planes(curl, at), w_z))
        put(c_y, at, along_columns(DERIV, u, -1))


def turn_z(temp, mass, curl, c_x, c_y):
    @pl.loop(0, 4)
    def _(z):
        at = lambda x, y: quad(x, y, z)
        u = along_columns(CLOSED, planes(temp, at))
        scale = planes(curl, at)
        w_y = times(scale, minus(planes(c_y, at), along_rows(DERIV, u, -1)))
        w_x = times(scale, plus(planes(c_x, at), along_columns(DERIV, u, -1)))
        put(c_y, at, w_y)
        put(c_x, at, w_x)
        v = times(planes(mass, at), u)
        v = plus(v, along_columns(DERIV.T, w_x, -1))
        v = minus(v, along_rows(DERIV.T, w_y, -1))
        put(temp, at, along_columns(CLOSED.T, v))


def finish_z(dofs, sign, temp):
    @pl.loop(0, 4)
    def _(b):
        values = along_rows(CLOSED.T, planes(temp, lambda x, z: quad(x, b, z)))
        store_plane(dofs, sign, rows_fixed_b(2, b), along_columns(OPENED.T, values))


def backward_x(dofs, sign, mass, temp, u_x, c_y, c_z):
    @pl.loop(0, 4)
    def _(x):
        at = lambda y, z: quad(x, y, z)
        v = times(planes(mass, at), planes(u_x, at))
        v = plus(v, along_columns(DERIV.T, planes(c_y, at), -1))
        v = minus(v, along_rows(DERIV.T, planes(c_z, at), -1))
        put(temp, at, along_rows(CLOSED.T, v))

    @pl.loop(0, 4)
    def _(b):
        values = along_columns(CLOSED.T, planes(temp, lambda x, z: quad(x, b, z)))
        store_plane(dofs, sign, rows_fixed_b(0, b), along_rows(OPENED.T, values))


def backward_y(dofs, sign, mass, temp, u_y, c_x, c_z):
    @pl.loop(0, 4)
    def _(y):
        at = lambda x, z: quad(x, y, z)
        v = times(planes(mass, at), planes(u_y, at))
        v = plus(v, along_rows(DERIV.T, planes(c_z, at), -1))
        v = minus(v, along_columns(DERIV.T, planes(c_x, at), -1))
        put(temp, at, along_rows(CLOSED.T, v))

    @pl.loop(0, 4)
    def _(a):
        values = along_columns(CLOSED.T, planes(temp, lambda y, z: quad(a, y, z)))
        store_plane(dofs, sign, rows_fixed_a(1, a), along_rows(OPENED.T, values))


def join_elements(dofs, comp):
    rows = lax.broadcasted_iota(jnp.int32, (8, LANES), 0)
    for axis, step in ((0, 2), (1, 1), (2, 4)):
        if comp == axis:
            continue
        upper = (rows // step) % 2 == 1
        sizes = [3 if comp == other else 4 for other in range(3)]
        sizes[axis] = 1
        for a in range(sizes[0]):
            for b in range(sizes[1]):
                for c in range(sizes[2]):
                    high = [a, b, c]
                    high[axis] = 3
                    to = pl.ds(row_of(comp, a, b, c), 8)
                    moved = pltpu.roll(dofs[pl.ds(row_of(comp, *high), 8), :], step, 0)
                    dofs[to, :] = dofs[to, :] + jnp.where(upper, moved, 0.0)


def scatter_own(vec, dofs):
    for comp in range(3):
        for x, i, a in places(comp, 0):
            for y, j, b in places(comp, 1):
                if x == 6 or y == 6:
                    continue
                for k in range(2):
                    count = 4 if comp != 2 and k == 0 else 3
                    at = row_of(comp, a, b, 0, element(i, j, k))
                    dofs[pl.ds(at, count, 8), :] = vec[comp, x, y, pl.ds(3 * k, count), :]


def scatter_line(dofs, comp, i, a, j, b, source):
    for k in range(2):
        count = 4 if comp != 2 and k == 0 else 3
        at = row_of(comp, a, b, 0, element(i, j, k))
        dofs[pl.ds(at, count, 8), :] = source(pl.ds(3 * k, count))


def scatter_xz_halo(dofs, r_x, r_z, r_e):
    for comp in (1, 2):
        for y, j, b in places(comp, 1):
            if y < 6:
                scatter_line(dofs, comp, 1, 3, j, b, lambda z: r_x[comp - 1, y, z, :])
    for x, i, a in places(0, 0):
        for j in range(2):
            count = 4 - j
            at = row_of(0, a, 0, 3, element(i, j, 1))
            dofs[pl.ds(at, count, 32), :] = r_z[0, x, pl.ds(3 * j, count), :]
    for x, i, a in places(1, 0):
        if x < 6:
            for j in range(2):
                at = row_of(1, a, 0, 3, element(i, j, 1))
                dofs[pl.ds(at, 3, 32), :] = r_z[1, x, pl.ds(3 * j, 3), :]
    for j in range(2):
        at = row_of(1, 3, 0, 3, element(1, j, 1))
        dofs[pl.ds(at, 3, 32), :] = r_e[1, pl.ds(3 * j, 3), :]


def scatter_y_halo(dofs, r_y, r_e):
    for comp in (0, 2):
        for x, i, a in places(comp, 0):
            if x < 6:
                scatter_line(dofs, comp, i, a, 1, 3, lambda z: r_y[comp // 2, x, z, :])
    for i in range(2):
        at = row_of(0, 0, 3, 3, element(i, 1, 1))
        dofs[pl.ds(at, 3, 128), :] = r_e[0, pl.ds(3 * i, 3), :]


def runs(comp, axis, fixed):
    local = [None if g is None else owners(comp, n)[g][1:] for n, g in enumerate(fixed)]
    result = []
    for half in range(2):
        count = 3 + half * (comp != axis)
        at = [(half, 0) if entry is None else entry for entry in local]
        (i, a), (j, b), (k, c) = at
        row = row_of(comp, a, b, c, element(i, j, k))
        result.append((pl.ds(3 * half, count), pl.ds(row, count, 8 * STRIDE[comp][axis])))
    return result


def owned(comp, axis):
    return range(6 if comp == axis else 7)


def to_grid(dofs, comp, out, line):
    other = 3 - line
    for x in owned(comp, 0):
        for q in owned(comp, other):
            fixed = [x, None, None]
            fixed[other] = q
            for grid, rows in runs(comp, line, fixed):
                out[x, q, grid, :] = dofs[rows, :]


def pack_face(dofs, comp, axis, line, pack):
    third = 3 - axis - line
    for side in range(2):
        for p in owned(comp, third):
            fixed = [None] * 3
            fixed[axis] = 6 * side
            fixed[third] = p
            for grid, rows in runs(comp, line, fixed):
                pack[side, p, grid, :] = dofs[rows, :]


def add_face(dofs, comp, axis, line, given):
    third = 3 - axis - line
    for side in range(2):
        for p in owned(comp, third):
            fixed = [None] * 3
            fixed[axis] = 6 * side
            fixed[third] = p
            for grid, rows in runs(comp, line, fixed):
                dofs[rows, :] = dofs[rows, :] + given[side, p, grid, :]


def edge_runs(comp, n):
    fixed = [None] * 3
    for axis, sign in zip(EDGE_AXES[comp], SIGNS[n]):
        fixed[axis] = 6 * (sign > 0)
    return runs(comp, comp, fixed)


def pack_edges(dofs, comp, edges):
    for n in range(4):
        for grid, rows in edge_runs(comp, n):
            edges[comp, n, grid, :] = dofs[rows, :]


def add_edges(dofs, comp, given):
    for n in range(4):
        for grid, rows in edge_runs(comp, n):
            dofs[rows, :] = dofs[rows, :] + given[comp, n, grid, :]


def kernel(
    sizes,
    vec_hbm,
    flip_hbm,
    rel_hbm,
    con_hbm,
    out_x,
    out_y,
    out_z,
    vec,
    flip,
    rel,
    con,
    flat,
    sign,
    mass,
    curl,
    dofs,
    temp,
    u_x,
    u_y,
    c_x,
    c_y,
    c_z,
    s_z,
    s_e,
    r_x,
    r_y,
    r_z,
    r_e,
    t_x,
    t_z,
    p_xy,
    p_xz,
    p_yx,
    p_yz,
    p_zx,
    p_zy,
    p_e,
    f_xy,
    f_xz,
    f_yx,
    f_yz,
    f_zx,
    f_zy,
    f_e,
    load_sem,
    send_sem,
    recv_sem,
):
    me = [lax.axis_index(axis) for axis in AXES]

    def neighbour(*steps):
        return tuple(lax.rem(me[n] + steps[n] + sizes[n], sizes[n]) for n in range(3))

    loads = [
        pltpu.make_async_copy(source, target, load_sem.at[n])
        for n, (source, target) in enumerate(
            ((vec_hbm, vec), (flip_hbm, flip), (rel_hbm, rel), (con_hbm, con))
        )
    ]
    for copy in loads:
        copy.start()

    barrier = pltpu.get_barrier_semaphore()
    upper = ((0, 1, 0), (1, 1, 0), (0, 1, 1), (1, 0, 0), (1, 0, 1), (0, 0, 1))
    for steps in upper:
        pl.semaphore_signal(barrier, inc=1, device_id=neighbour(*steps), device_id_type=MESH)

    copies = []

    def send(source, target, *steps):
        n = len(copies)
        copy = pltpu.make_async_remote_copy(
            src_ref=source,
            dst_ref=target,
            send_sem=send_sem.at[n],
            recv_sem=recv_sem.at[n],
            device_id=neighbour(*steps),
            device_id_type=MESH,
        )
        copy.start()
        copies.append(copy)
        return copy

    def send_faces(axis, pack, target):
        faces = []
        for side in range(2):
            steps = [(2 * side - 1) * (axis == n) for n in range(3)]
            faces.append(send(pack.at[side], target.at[1 - side], *steps))
        return faces

    def send_edges(comp):
        sent = []
        for n, pair in enumerate(SIGNS):
            steps = [0, 0, 0]
            for axis, step in zip(EDGE_AXES[comp], pair):
                steps[axis] = step
            sent.append(send(p_e.at[comp, n], f_e.at[comp, 3 - n], *steps))
        return sent

    def receive(arriving):
        for copy in arriving:
            copy.wait_recv()

    loads[0].wait()
    for comp in range(2):
        for x in range(6):
            for y in range(6):
                s_z[comp, x, pl.ds(y, 1), :] = vec[comp, x, y, pl.ds(0, 1), :]
    for n in range(6):
        s_e[0, pl.ds(n, 1), :] = vec[0, n, 0, pl.ds(0, 1), :]
        s_e[1, pl.ds(n, 1), :] = vec[1, 0, n, pl.ds(0, 1), :]
    pl.semaphore_wait(barrier, len(upper))
    xy_halo = [send(vec.at[2, 0, 0], r_e.at[2], -1, -1, 0)]
    y_halo = [
        send(s_e.at[0], r_e.at[0], 0, -1, -1),
        send(vec.at[0, :, 0], r_y.at[0], 0, -1, 0),
        send(vec.at[2, :, 0], r_y.at[1], 0, -1, 0),
    ]
    xz_halo = [
        send(s_e.at[1], r_e.at[1], -1, 0, -1),
        send(vec.at[pl.ds(1, 2), 0], r_x, -1, 0, 0),
        send(s_z, r_z, 0, 0, -1),
    ]

    scatter_own(vec, dofs)
    for copy in loads[1:]:
        copy.wait()
    prepare(flip, rel, con, flat, sign, mass, curl)
    receive(xz_halo)
    scatter_xz_halo(dofs, r_x, r_z, r_e)
    forward_y(dofs, sign, temp, u_y, c_x, c_z)

    @pl.loop(0, 3)
    def _(b):
        start_x(dofs, sign, t_x, b)
        start_z(dofs, sign, t_z, b)

    receive(y_halo)
    scatter_y_halo(dofs, r_y, r_e)
    start_x(dofs, sign, t_x, 3)
    forward_x(t_x, curl, u_x, c_y, c_z)
    receive(xy_halo)
    scatter_line(dofs, 2, 1, 3, 1, 3, lambda z: r_e[2, z, :])
    start_z(dofs, sign, t_z, 3)
    turn_z(t_z, mass, curl, c_x, c_y)
    finish_z(dofs, sign, t_z)
    join_elements(dofs, 2)
    pack_edges(dofs, 2, p_e)
    edges_z = send_edges(2)
    pack_face(dofs, 2, 1, 2, p_yz)
    faces_yz = send_faces(1, p_yz, f_yz)
    pack_face(dofs, 2, 0, 1, p_xz)
    faces_xz = send_faces(0, p_xz, f_xz)

    backward_x(dofs, sign, mass, t_x, u_x, c_y, c_z)
    join_elements(dofs, 0)
    pack_edges(dofs, 0, p_e)
    edges_x = send_edges(0)
    pack_face(dofs, 0, 1, 2, p_yx)
    faces_yx = send_faces(1, p_yx, f_yx)
    pack_face(dofs, 0, 2, 1, p_zx)
    faces_zx = send_faces(2, p_zx, f_zx)

    backward_y(dofs, sign, mass, temp, u_y, c_x, c_z)
    join_elements(dofs, 1)
    pack_edges(dofs, 1, p_e)
    edges_y = send_edges(1)
    pack_face(dofs, 1, 0, 2, p_xy)
    faces_xy = send_faces(0, p_xy, f_xy)
    pack_face(dofs, 1, 2, 1, p_zy)
    faces_zy = send_faces(2, p_zy, f_zy)

    receive(faces_zx)
    add_face(dofs, 0, 2, 1, f_zx)
    to_grid(dofs, 0, out_x, 2)
    receive(faces_yz + edges_z)
    add_face(dofs, 2, 1, 2, f_yz)
    add_edges(dofs, 2, f_e)
    to_grid(dofs, 2, out_z, 1)
    receive(faces_xz)
    for side in range(2):
        out_z[6 * side] = out_z[6 * side] + f_xz[side]
    receive(faces_zy + edges_y)
    add_face(dofs, 1, 2, 1, f_zy)
    add_edges(dofs, 1, f_e)
    to_grid(dofs, 1, out_y, 2)
    receive(faces_xy)
    for side in range(2):
        out_y[6 * side] = out_y[6 * side] + f_xy[side]
    receive(edges_x)
    for n, pair in enumerate(SIGNS):
        y, z = 6 * (pair[0] > 0), 6 * (pair[1] > 0)
        for x in range(6):
            at = pl.ds(z, 1)
            out_x[x, y, at, :] = out_x[x, y, at, :] + f_e[0, n, pl.ds(x, 1), :]
    receive(faces_yx)
    for side in range(2):
        for x in range(6):
            out_x[x, 6 * side] = out_x[x, 6 * side] + f_yx[side, x]
    for copy in copies:
        copy.wait_send()


def put_out(in_x, in_y, in_z, out_x, out_y, out_z, sem):
    pairs = ((in_x, out_x), (in_y, out_y), (in_z, out_z))
    copies = [pltpu.make_async_copy(*pair, sem.at[n]) for n, pair in enumerate(pairs)]
    for copy in copies:
        copy.start()
    for copy in copies:
        copy.wait()


def on_device(sizes, vectors, orient_flip, reluctivity, conductivity):
    f32 = jnp.float32
    regs = lambda n: pltpu.VMEM((n, 8, LANES), f32)
    grid = ((6, 7, 7, LANES), (7, 6, 7, LANES), (7, 6, 7, LANES))
    faces = [
        pltpu.VMEM(shape, f32)
        for shape in (
            (2, 6, 7, LANES),
            (2, 6, 7, LANES),
            (2, 6, 7, LANES),
            (2, 7, 6, LANES),
            (2, 6, 7, LANES),
            (2, 7, 6, LANES),
            (3, 4, 6, LANES),
        )
    ]
    results = pl.pallas_call(
        lambda *refs: kernel(sizes, *refs),
        out_shape=[pltpu.VMEM(shape, f32) for shape in grid],
        in_specs=[pl.BlockSpec(memory_space=pl.ANY)] * 4,
        out_specs=[pl.BlockSpec(memory_space=pltpu.VMEM)] * 3,
        scratch_shapes=[
            pltpu.VMEM((3, 6, 6, 6, LANES), f32),
            pltpu.VMEM(orient_flip.shape, jnp.int32),
            pltpu.VMEM(reluctivity.shape, f32),
            pltpu.VMEM(conductivity.shape, f32),
            pltpu.VMEM((8, 512), f32),
            regs(DOFS),
            regs(QPTS),
            regs(QPTS),
            pltpu.VMEM((8 * DOFS, LANES), f32),
            regs(QPTS),
            regs(QPTS),
            regs(QPTS),
            regs(QPTS),
            regs(QPTS),
            regs(QPTS),
            pltpu.VMEM((2, 6, 6, LANES), f32),
            pltpu.VMEM((2, 6, LANES), f32),
            pltpu.VMEM((2, 6, 6, LANES), f32),
            pltpu.VMEM((2, 6, 6, LANES), f32),
            pltpu.VMEM((2, 6, 6, LANES), f32),
            pltpu.VMEM((3, 6, LANES), f32),
            regs(QPTS),
            regs(QPTS),
            *faces,
            *faces,
            pltpu.SemaphoreType.DMA((4,)),
            pltpu.SemaphoreType.DMA((31,)),
            pltpu.SemaphoreType.DMA((31,)),
        ],
        compiler_params=pltpu.CompilerParams(collective_id=0, has_side_effects=True),
        name="curlcurl",
    )(vectors, orient_flip, reluctivity, conductivity)
    results = [pltpu.with_memory_space_constraint(result, pltpu.VMEM) for result in results]
    out_x, out_y, out_z = pl.pallas_call(
        put_out,
        out_shape=[jax.ShapeDtypeStruct(shape, f32) for shape in grid],
        in_specs=[pl.BlockSpec(memory_space=pltpu.VMEM)] * 3,
        out_specs=[pl.BlockSpec(memory_space=pl.ANY)] * 3,
        scratch_shapes=[pltpu.SemaphoreType.DMA((3,))],
        name="putout",
    )(*results)
    return (out_x, out_y, jnp.swapaxes(out_z, 1, 2))


def solution(mesh):
    sizes = tuple(mesh.shape[axis] for axis in AXES)
    return jax.shard_map(
        lambda *args: on_device(sizes, *args),
        mesh=mesh,
        in_specs=(
            P(None, "gx", "gy", "gz", None),
            P("gx", "gy", "gz"),
            P("gx", "gy", "gz"),
            P("gx", "gy", "gz"),
        ),
        out_specs=(P("gx", "gy", "gz", None), P("gx", "gy", "gz", None), P("gx", "gy", "gz", None)),
        check_vma=False,
    )
```

```python
import jax
import jax.numpy as jnp
import numpy as np
from jax import lax
from jax.experimental import pallas as pl
from jax.experimental.pallas import tpu as pltpu
from jax.sharding import PartitionSpec as P

MESH = pl.DeviceIdType.MESH
AXES = ("gx", "gy", "gz")
LANES = 128
DOFS = 144
QPTS = 64
BASE = (0, 48, 96)
STRIDE = ((16, 4, 1), (12, 4, 1), (12, 3, 1))
EDGE_AXES = ((1, 2), (0, 2), (0, 1))
SIGNS = ((-1, -1), (-1, 1), (1, -1), (1, 1))


def lagrange(points_at, evaluate_at):
    amount = len(points_at)
    values = np.ones((len(evaluate_at), amount))
    slopes = np.zeros((len(evaluate_at), amount))
    for which in range(amount):
        for column in range(amount):
            if column != which:
                factor = (evaluate_at - points_at[column]) / (points_at[which] - points_at[column])
                slopes[:, which] = slopes[:, which] * factor + values[:, which] / (
                    points_at[which] - points_at[column]
                )
                values[:, which] = values[:, which] * factor
    return (values, slopes)


def basis_tables():
    lobatto = np.array([0.0, (1 - 5 ** (-0.5)) / 2, (1 + 5 ** (-0.5)) / 2, 1.0])
    gauss_open = np.array([(1 - 0.6**0.5) / 2, 0.5, (1 + 0.6**0.5) / 2])
    inner_pt = (3.0 / 7 - 2.0 / 7 * (6.0 / 5) ** 0.5) ** 0.5
    outer_pt = (3.0 / 7 + 2.0 / 7 * (6.0 / 5) ** 0.5) ** 0.5
    inner_wt = (18 + 30**0.5) / 36
    outer_wt = (18 - 30**0.5) / 36
    quad_points = (1 + np.array([-outer_pt, -inner_pt, inner_pt, outer_pt])) / 2
    quad_weight = np.array([outer_wt, inner_wt, inner_wt, outer_wt]) / 2
    closed, slopes = lagrange(lobatto, quad_points)
    opened, unused_slopes = lagrange(gauss_open, quad_points)
    return (closed, slopes, opened, quad_weight)


CLOSED, SLOPES, OPENED, WEIGHT = basis_tables()
DERIV = SLOPES @ np.linalg.inv(CLOSED)


def apply(table, given, parity):
    rows, columns = table.shape
    half = columns // 2
    sums = [given[c] + given[columns - 1 - c] for c in range(half)]
    diffs = [given[c] - given[columns - 1 - c] for c in range(half)]
    result = [None] * rows
    for q in range((rows + 1) // 2):
        even = None
        for c in range(half):
            term = sums[c] * float((table[q, c] + table[q, columns - 1 - c]) / 2)
            even = term if even is None else even + term
        if columns % 2:
            even = even + given[half] * float(table[q, half])
        if 2 * q + 1 == rows:
            result[q] = even
            continue
        odd = None
        for c in range(half):
            term = diffs[c] * float((table[q, c] - table[q, columns - 1 - c]) / 2)
            odd = term if odd is None else odd + term
        result[q] = even + odd
        result[rows - 1 - q] = even - odd if parity > 0 else odd - even
    return result


def along_rows(table, plane, parity=1):
    columns = [apply(table, [row[c] for row in plane], parity) for c in range(len(plane[0]))]
    return [[column[q] for column in columns] for q in range(table.shape[0])]


def along_columns(table, plane, parity=1):
    return [apply(table, row, parity) for row in plane]


def combine(op, *planes):
    return [[op(*entries) for entries in zip(*rows)] for rows in zip(*planes)]


def plus(p, q):
    return combine(lambda s, t: s + t, p, q)


def minus(p, q):
    return combine(lambda s, t: s - t, p, q)


def times(p, q):
    return combine(lambda s, t: s * t, p, q)


def dof(comp, a, b, c):
    s = STRIDE[comp]
    return BASE[comp] + a * s[0] + b * s[1] + c * s[2]


def row_of(comp, a, b, c, element=0):
    return 8 * dof(comp, a, b, c) + element


def element(i, j, k):
    return 4 * k + 2 * i + j


def places(comp, axis):
    if comp == axis:
        return [(g, g // 3, g % 3) for g in range(6)]
    return [(g, 0, g) for g in range(4)] + [(g, 1, g - 3) for g in range(3, 7)]


def owners(comp, axis):
    last = 6 if comp == axis else 7
    return [(g, min(g // 3, 1), g - 3 * min(g // 3, 1)) for g in range(last)]


def prepare(flip, rel, con, flat, sign, mass, curl):
    for k in range(2):
        for i in range(2):
            at = pl.ds(4 * k + 2 * i, 2)
            flat[at, 0:DOFS] = 1.0 - 2.0 * flip[i][:, DOFS * k : DOFS * (k + 1)].astype(jnp.float32)
            flat[at, 256 : 256 + QPTS] = rel[i][:, QPTS * k : QPTS * (k + 1)]
            flat[at, 384 : 384 + QPTS] = con[i][:, QPTS * k : QPTS * (k + 1)]
    whole = flat[:, 0:DOFS]
    for d in range(DOFS):
        sign[d] = jnp.broadcast_to(whole[:, d : d + 1], (8, LANES))
    rel_all = flat[:, 256 : 256 + QPTS]
    con_all = flat[:, 384 : 384 + QPTS]
    for q in range(QPTS):
        weight = float(WEIGHT[q // 16] * WEIGHT[q // 4 % 4] * WEIGHT[q % 4])
        curl[q] = jnp.broadcast_to(rel_all[:, q : q + 1], (8, LANES)) * weight
        mass[q] = jnp.broadcast_to(con_all[:, q : q + 1], (8, LANES)) * weight


def quad(x, y, z):
    return 16 * x + 4 * y + z


def planes(ref, at):
    return [[ref[at(p, q)] for q in range(4)] for p in range(4)]


def put(ref, at, plane):
    for p, row in enumerate(plane):
        for q, value in enumerate(row):
            ref[at(p, q)] = value


def load_plane(dofs, sign, rows):
    return [
        [dofs[pl.ds(pl.multiple_of(8 * d, 8), 8), :] * sign[d] for d in row] for row in rows
    ]


def store_plane(dofs, sign, rows, plane):
    for row, values in zip(rows, plane):
        for d, value in zip(row, values):
            dofs[pl.ds(pl.multiple_of(8 * d, 8), 8), :] = value * sign[d]


def rows_fixed_b(comp, b):
    return [[dof(comp, a, b, c) for c in range(4 - (comp == 2))] for a in range(4 - (comp == 0))]


def rows_fixed_a(comp, a):
    return [[dof(comp, a, b, c) for c in range(4)] for b in range(3)]


def forward_y(dofs, sign, temp, u_y, c_x, c_z):
    @pl.loop(0, 4, unroll=2)
    def _(a):
        values = along_rows(OPENED, load_plane(dofs, sign, rows_fixed_a(1, a)))
        put(temp, lambda y, z: quad(a, y, z), along_columns(CLOSED, values))

    @pl.loop(0, 4, unroll=2)
    def _(y):
        at = lambda x, z: quad(x, y, z)
        u = along_rows(CLOSED, planes(temp, at))
        put(u_y, at, u)
        put(c_z, at, along_rows(DERIV, u, -1))
        put(c_x, at, along_columns(-DERIV, u, -1))


def start_x(dofs, sign, temp, b):
    values = along_rows(OPENED, load_plane(dofs, sign, rows_fixed_b(0, b)))
    put(temp, lambda x, z: quad(x, b, z), along_columns(CLOSED, values))


def start_z(dofs, sign, temp, b):
    values = along_columns(OPENED, load_plane(dofs, sign, rows_fixed_b(2, b)))
    put(temp, lambda x, z: quad(x, b, z), along_rows(CLOSED, values))


def forward_x(temp, curl, u_x, c_y, c_z):
    @pl.loop(0, 4, unroll=2)
    def _(x):
        at = lambda y, z: quad(x, y, z)
        u = along_rows(CLOSED, planes(temp, at))
        put(u_x, at, u)
        w_z = minus(planes(c_z, at), along_rows(DERIV, u, -1))
        put(c_z, at, times(planes(curl, at), w_z))
        put(c_y, at, along_columns(DERIV, u, -1))


def turn_z(temp, mass, curl, c_x, c_y):
    @pl.loop(0, 4, unroll=2)
    def _(z):
        at = lambda x, y: quad(x, y, z)
        u = along_columns(CLOSED, planes(temp, at))
        scale = planes(curl, at)
        w_y = times(scale, minus(planes(c_y, at), along_rows(DERIV, u, -1)))
        w_x = times(scale, plus(planes(c_x, at), along_columns(DERIV, u, -1)))
        put(c_y, at, w_y)
        put(c_x, at, w_x)
        v = times(planes(mass, at), u)
        v = plus(v, along_columns(DERIV.T, w_x, -1))
        v = minus(v, along_rows(DERIV.T, w_y, -1))
        put(temp, at, along_columns(CLOSED.T, v))


def finish_z(dofs, sign, temp):
    @pl.loop(0, 4, unroll=2)
    def _(b):
        values = along_rows(CLOSED.T, planes(temp, lambda x, z: quad(x, b, z)))
        store_plane(dofs, sign, rows_fixed_b(2, b), along_columns(OPENED.T, values))


def backward_x(dofs, sign, mass, temp, u_x, c_y, c_z):
    @pl.loop(0, 4, unroll=2)
    def _(x):
        at = lambda y, z: quad(x, y, z)
        v = times(planes(mass, at), planes(u_x, at))
        v = plus(v, along_columns(DERIV.T, planes(c_y, at), -1))
        v = minus(v, along_rows(DERIV.T, planes(c_z, at), -1))
        put(temp, at, along_rows(CLOSED.T, v))

    @pl.loop(0, 4, unroll=2)
    def _(b):
        values = along_columns(CLOSED.T, planes(temp, lambda x, z: quad(x, b, z)))
        store_plane(dofs, sign, rows_fixed_b(0, b), along_rows(OPENED.T, values))


def backward_y(dofs, sign, mass, temp, u_y, c_x, c_z):
    @pl.loop(0, 4, unroll=2)
    def _(y):
        at = lambda x, z: quad(x, y, z)
        v = times(planes(mass, at), planes(u_y, at))
        v = plus(v, along_rows(DERIV.T, planes(c_z, at), -1))
        v = minus(v, along_columns(DERIV.T, planes(c_x, at), -1))
        put(temp, at, along_rows(CLOSED.T, v))

    @pl.loop(0, 4, unroll=2)
    def _(a):
        values = along_columns(CLOSED.T, planes(temp, lambda y, z: quad(a, y, z)))
        store_plane(dofs, sign, rows_fixed_a(1, a), along_rows(OPENED.T, values))


def join_elements(dofs, comp):
    rows = lax.broadcasted_iota(jnp.int32, (8, LANES), 0)
    for axis, step in ((0, 2), (1, 1), (2, 4)):
        if comp == axis:
            continue
        upper = (rows // step) % 2 == 1
        sizes = [3 if comp == other else 4 for other in range(3)]
        sizes[axis] = 1
        for a in range(sizes[0]):
            for b in range(sizes[1]):
                for c in range(sizes[2]):
                    high = [a, b, c]
                    high[axis] = 3
                    to = pl.ds(row_of(comp, a, b, c), 8)
                    moved = pltpu.roll(dofs[pl.ds(row_of(comp, *high), 8), :], step, 0)
                    dofs[to, :] = dofs[to, :] + jnp.where(upper, moved, 0.0)


def scatter_own(vec, dofs):
    for comp in range(3):
        for x, i, a in places(comp, 0):
            for y, j, b in places(comp, 1):
                if x == 6 or y == 6:
                    continue
                for k in range(2):
                    count = 4 if comp != 2 and k == 0 else 3
                    at = row_of(comp, a, b, 0, element(i, j, k))
                    dofs[pl.ds(at, count, 8), :] = vec[comp, x, y, pl.ds(3 * k, count), :]


def scatter_line(dofs, comp, i, a, j, b, source):
    for k in range(2):
        count = 4 if comp != 2 and k == 0 else 3
        at = row_of(comp, a, b, 0, element(i, j, k))
        dofs[pl.ds(at, count, 8), :] = source(pl.ds(3 * k, count))


def scatter_xz_halo(dofs, r_x, r_z):
    for comp in (1, 2):
        for y, j, b in places(comp, 1):
            if y < 6:
                scatter_line(dofs, comp, 1, 3, j, b, lambda z: r_x[comp - 1, y, z, :])
    for x, i, a in places(0, 0):
        for j in range(2):
            count = 4 - j
            at = row_of(0, a, 0, 3, element(i, j, 1))
            dofs[pl.ds(at, count, 32), :] = r_z[0, x, pl.ds(3 * j, count), :]
    for x, i, a in places(1, 0):
        if x < 6:
            for j in range(2):
                at = row_of(1, a, 0, 3, element(i, j, 1))
                dofs[pl.ds(at, 3, 32), :] = r_z[1, x, pl.ds(3 * j, 3), :]


def scatter_xz_edge(dofs, r_e):
    for j in range(2):
        at = row_of(1, 3, 0, 3, element(1, j, 1))
        dofs[pl.ds(at, 3, 32), :] = r_e[1, pl.ds(3 * j, 3), :]


def scatter_y_halo(dofs, r_y, r_e):
    for comp in (0, 2):
        for x, i, a in places(comp, 0):
            if x < 6:
                scatter_line(dofs, comp, i, a, 1, 3, lambda z: r_y[comp // 2, x, z, :])
    for i in range(2):
        at = row_of(0, 0, 3, 3, element(i, 1, 1))
        dofs[pl.ds(at, 3, 128), :] = r_e[0, pl.ds(3 * i, 3), :]


def runs(comp, axis, fixed):
    local = [None if g is None else owners(comp, n)[g][1:] for n, g in enumerate(fixed)]
    result = []
    for half in range(2):
        count = 3 + half * (comp != axis)
        at = [(half, 0) if entry is None else entry for entry in local]
        (i, a), (j, b), (k, c) = at
        row = row_of(comp, a, b, c, element(i, j, k))
        result.append((pl.ds(3 * half, count), pl.ds(row, count, 8 * STRIDE[comp][axis])))
    return result


def owned(comp, axis):
    return range(6 if comp == axis else 7)


def to_grid(dofs, comp, out, line):
    other = 3 - line
    for x in owned(comp, 0):
        for q in owned(comp, other):
            fixed = [x, None, None]
            fixed[other] = q
            for grid, rows in runs(comp, line, fixed):
                out[x, q, grid, :] = dofs[rows, :]


def pack_face(dofs, comp, axis, line, pack):
    third = 3 - axis - line
    for side in range(2):
        for p in owned(comp, third):
            fixed = [None] * 3
            fixed[axis] = 6 * side
            fixed[third] = p
            for grid, rows in runs(comp, line, fixed):
                pack[side, p, grid, :] = dofs[rows, :]


def add_face(dofs, comp, axis, line, given):
    third = 3 - axis - line
    for side in range(2):
        for p in owned(comp, third):
            fixed = [None] * 3
            fixed[axis] = 6 * side
            fixed[third] = p
            for grid, rows in runs(comp, line, fixed):
                dofs[rows, :] = dofs[rows, :] + given[side, p, grid, :]


def edge_runs(comp, n):
    fixed = [None] * 3
    for axis, sign in zip(EDGE_AXES[comp], SIGNS[n]):
        fixed[axis] = 6 * (sign > 0)
    return runs(comp, comp, fixed)


def pack_edges(dofs, comp, edges):
    for n in range(4):
        for grid, rows in edge_runs(comp, n):
            edges[comp, n, grid, :] = dofs[rows, :]


def add_edges(dofs, comp, given):
    for n in range(4):
        for grid, rows in edge_runs(comp, n):
            dofs[rows, :] = dofs[rows, :] + given[comp, n, grid, :]


def kernel(
    sizes,
    vec_hbm,
    flip_hbm,
    rel_hbm,
    con_hbm,
    out_x,
    out_y,
    out_z,
    vec,
    flip,
    rel,
    con,
    flat,
    sign,
    mass,
    curl,
    dofs,
    temp,
    u_x,
    u_y,
    c_x,
    c_y,
    c_z,
    s_z,
    s_e,
    r_x,
    r_y,
    r_z,
    r_e,
    t_x,
    t_z,
    p_xy,
    p_xz,
    p_yx,
    p_yz,
    p_zx,
    p_zy,
    p_e,
    f_xy,
    f_xz,
    f_yx,
    f_yz,
    f_zx,
    f_zy,
    f_e,
    load_sem,
    send_sem,
    recv_sem,
):
    me = [lax.axis_index(axis) for axis in AXES]

    def neighbour(*steps):
        return tuple(lax.rem(me[n] + steps[n] + sizes[n], sizes[n]) for n in range(3))

    loads = [
        pltpu.make_async_copy(source, target, load_sem.at[n])
        for n, (source, target) in enumerate(
            ((vec_hbm, vec), (flip_hbm, flip), (rel_hbm, rel), (con_hbm, con))
        )
    ]
    for copy in loads:
        copy.start()

    barrier = pltpu.get_barrier_semaphore()
    upper = ((0, 1, 0), (1, 1, 0), (0, 1, 1), (1, 0, 0), (1, 0, 1), (0, 0, 1))
    for steps in upper:
        pl.semaphore_signal(barrier, inc=1, device_id=neighbour(*steps), device_id_type=MESH)

    copies = []

    def send(source, target, *steps):
        n = len(copies)
        copy = pltpu.make_async_remote_copy(
            src_ref=source,
            dst_ref=target,
            send_sem=send_sem.at[n],
            recv_sem=recv_sem.at[n],
            device_id=neighbour(*steps),
            device_id_type=MESH,
        )
        copy.start()
        copies.append(copy)
        return copy

    def send_faces(axis, pack, target):
        faces = []
        for side in range(2):
            steps = [(2 * side - 1) * (axis == n) for n in range(3)]
            faces.append(send(pack.at[side], target.at[1 - side], *steps))
        return faces

    def send_edges(comp):
        sent = []
        for n, pair in enumerate(SIGNS):
            steps = [0, 0, 0]
            for axis, step in zip(EDGE_AXES[comp], pair):
                steps[axis] = step
            sent.append(send(p_e.at[comp, n], f_e.at[comp, 3 - n], *steps))
        return sent

    def receive(arriving):
        for copy in arriving:
            copy.wait_recv()

    loads[0].wait()
    for comp in range(2):
        for x in range(6):
            for y in range(6):
                s_z[comp, x, pl.ds(y, 1), :] = vec[comp, x, y, pl.ds(0, 1), :]
    for n in range(6):
        s_e[0, pl.ds(n, 1), :] = vec[0, n, 0, pl.ds(0, 1), :]
        s_e[1, pl.ds(n, 1), :] = vec[1, 0, n, pl.ds(0, 1), :]
    pl.semaphore_wait(barrier, len(upper))
    xy_halo = [send(vec.at[2, 0, 0], r_e.at[2], -1, -1, 0)]
    y_halo = [
        send(s_e.at[0], r_e.at[0], 0, -1, -1),
        send(vec.at[0, :, 0], r_y.at[0], 0, -1, 0),
        send(vec.at[2, :, 0], r_y.at[1], 0, -1, 0),
    ]
    xz_halo = [
        send(s_e.at[1], r_e.at[1], -1, 0, -1),
        send(vec.at[pl.ds(1, 2), 0], r_x, -1, 0, 0),
        send(s_z, r_z, 0, 0, -1),
    ]

    scatter_own(vec, dofs)
    for copy in loads[1:]:
        copy.wait()
    prepare(flip, rel, con, flat, sign, mass, curl)
    receive(xz_halo[1:])
    scatter_xz_halo(dofs, r_x, r_z)

    @pl.loop(0, 3, unroll=1)
    def _(b):
        start_x(dofs, sign, t_x, b)
        start_z(dofs, sign, t_z, b)

    receive(xz_halo[:1])
    scatter_xz_edge(dofs, r_e)
    forward_y(dofs, sign, temp, u_y, c_x, c_z)
    receive(y_halo)
    scatter_y_halo(dofs, r_y, r_e)
    start_x(dofs, sign, t_x, 3)
    forward_x(t_x, curl, u_x, c_y, c_z)
    receive(xy_halo)
    scatter_line(dofs, 2, 1, 3, 1, 3, lambda z: r_e[2, z, :])
    start_z(dofs, sign, t_z, 3)
    turn_z(t_z, mass, curl, c_x, c_y)
    finish_z(dofs, sign, t_z)
    join_elements(dofs, 2)
    pack_edges(dofs, 2, p_e)
    edges_z = send_edges(2)
    pack_face(dofs, 2, 1, 2, p_yz)
    faces_yz = send_faces(1, p_yz, f_yz)
    pack_face(dofs, 2, 0, 1, p_xz)
    faces_xz = send_faces(0, p_xz, f_xz)

    backward_x(dofs, sign, mass, t_x, u_x, c_y, c_z)
    join_elements(dofs, 0)
    pack_edges(dofs, 0, p_e)
    edges_x = send_edges(0)
    pack_face(dofs, 0, 1, 2, p_yx)
    faces_yx = send_faces(1, p_yx, f_yx)
    pack_face(dofs, 0, 2, 1, p_zx)
    faces_zx = send_faces(2, p_zx, f_zx)

    backward_y(dofs, sign, mass, temp, u_y, c_x, c_z)
    join_elements(dofs, 1)
    pack_edges(dofs, 1, p_e)
    edges_y = send_edges(1)
    pack_face(dofs, 1, 0, 2, p_xy)
    faces_xy = send_faces(0, p_xy, f_xy)
    pack_face(dofs, 1, 2, 1, p_zy)
    faces_zy = send_faces(2, p_zy, f_zy)

    receive(faces_zx)
    add_face(dofs, 0, 2, 1, f_zx)
    to_grid(dofs, 0, out_x, 2)
    receive(faces_yz + edges_z)
    add_face(dofs, 2, 1, 2, f_yz)
    add_edges(dofs, 2, f_e)
    to_grid(dofs, 2, out_z, 1)
    receive(faces_xz)
    for side in range(2):
        out_z[6 * side] = out_z[6 * side] + f_xz[side]
    receive(faces_zy + edges_y)
    add_face(dofs, 1, 2, 1, f_zy)
    add_edges(dofs, 1, f_e)
    to_grid(dofs, 1, out_y, 2)
    receive(faces_xy)
    for side in range(2):
        out_y[6 * side] = out_y[6 * side] + f_xy[side]
    receive(edges_x)
    for n, pair in enumerate(SIGNS):
        y, z = 6 * (pair[0] > 0), 6 * (pair[1] > 0)
        for x in range(6):
            at = pl.ds(z, 1)
            out_x[x, y, at, :] = out_x[x, y, at, :] + f_e[0, n, pl.ds(x, 1), :]
    receive(faces_yx)
    for side in range(2):
        for x in range(6):
            out_x[x, 6 * side] = out_x[x, 6 * side] + f_yx[side, x]
    for copy in copies:
        copy.wait_send()


def put_out(in_x, in_y, in_z, out_x, out_y, out_z, sem):
    pairs = ((in_x, out_x), (in_y, out_y), (in_z, out_z))
    copies = [pltpu.make_async_copy(*pair, sem.at[n]) for n, pair in enumerate(pairs)]
    for copy in copies:
        copy.start()
    for copy in copies:
        copy.wait()


def on_device(sizes, vectors, orient_flip, reluctivity, conductivity):
    f32 = jnp.float32
    regs = lambda n: pltpu.VMEM((n, 8, LANES), f32)
    grid = ((6, 7, 7, LANES), (7, 6, 7, LANES), (7, 6, 7, LANES))
    faces = [
        pltpu.VMEM(shape, f32)
        for shape in (
            (2, 6, 7, LANES),
            (2, 6, 7, LANES),
            (2, 6, 7, LANES),
            (2, 7, 6, LANES),
            (2, 6, 7, LANES),
            (2, 7, 6, LANES),
            (3, 4, 6, LANES),
        )
    ]
    results = pl.pallas_call(
        lambda *refs: kernel(sizes, *refs),
        out_shape=[pltpu.VMEM(shape, f32) for shape in grid],
        in_specs=[pl.BlockSpec(memory_space=pl.ANY)] * 4,
        out_specs=[pl.BlockSpec(memory_space=pltpu.VMEM)] * 3,
        scratch_shapes=[
            pltpu.VMEM((3, 6, 6, 6, LANES), f32),
            pltpu.VMEM(orient_flip.shape, jnp.int32),
            pltpu.VMEM(reluctivity.shape, f32),
            pltpu.VMEM(conductivity.shape, f32),
            pltpu.VMEM((8, 512), f32),
            regs(DOFS),
            regs(QPTS),
            regs(QPTS),
            pltpu.VMEM((8 * DOFS, LANES), f32),
            regs(QPTS),
            regs(QPTS),
            regs(QPTS),
            regs(QPTS),
            regs(QPTS),
            regs(QPTS),
            pltpu.VMEM((2, 6, 6, LANES), f32),
            pltpu.VMEM((2, 6, LANES), f32),
            pltpu.VMEM((2, 6, 6, LANES), f32),
            pltpu.VMEM((2, 6, 6, LANES), f32),
            pltpu.VMEM((2, 6, 6, LANES), f32),
            pltpu.VMEM((3, 6, LANES), f32),
            regs(QPTS),
            regs(QPTS),
            *faces,
            *faces,
            pltpu.SemaphoreType.DMA((4,)),
            pltpu.SemaphoreType.DMA((31,)),
            pltpu.SemaphoreType.DMA((31,)),
        ],
        compiler_params=pltpu.CompilerParams(collective_id=0, has_side_effects=True),
        name="curlcurl",
    )(vectors, orient_flip, reluctivity, conductivity)
    results = [pltpu.with_memory_space_constraint(result, pltpu.VMEM) for result in results]
    out_x, out_y, out_z = pl.pallas_call(
        put_out,
        out_shape=[jax.ShapeDtypeStruct(shape, f32) for shape in grid],
        in_specs=[pl.BlockSpec(memory_space=pltpu.VMEM)] * 3,
        out_specs=[pl.BlockSpec(memory_space=pl.ANY)] * 3,
        scratch_shapes=[pltpu.SemaphoreType.DMA((3,))],
        name="putout",
    )(*results)
    return (out_x, out_y, jnp.swapaxes(out_z, 1, 2))


def solution(mesh):
    sizes = tuple(mesh.shape[axis] for axis in AXES)
    return jax.shard_map(
        lambda *args: on_device(sizes, *args),
        mesh=mesh,
        in_specs=(
            P(None, "gx", "gy", "gz", None),
            P("gx", "gy", "gz"),
            P("gx", "gy", "gz"),
            P("gx", "gy", "gz"),
        ),
        out_specs=(P("gx", "gy", "gz", None), P("gx", "gy", "gz", None), P("gx", "gy", "gz", None)),
        check_vma=False,
    )
```

```python
import jax
import jax.numpy as jnp
import numpy as np
from jax import lax
from jax.experimental import pallas as pl
from jax.experimental.pallas import tpu as pltpu
from jax.sharding import PartitionSpec as P

MESH = pl.DeviceIdType.MESH
AXES = ("gx", "gy", "gz")
LANES = 128
DOFS = 144
QPTS = 64
BASE = (0, 48, 96)
STRIDE = ((16, 4, 1), (12, 4, 1), (12, 3, 1))
EDGE_AXES = ((1, 2), (0, 2), (0, 1))
SIGNS = ((-1, -1), (-1, 1), (1, -1), (1, 1))


def lagrange(points_at, evaluate_at):
    amount = len(points_at)
    values = np.ones((len(evaluate_at), amount))
    slopes = np.zeros((len(evaluate_at), amount))
    for which in range(amount):
        for column in range(amount):
            if column != which:
                factor = (evaluate_at - points_at[column]) / (points_at[which] - points_at[column])
                slopes[:, which] = slopes[:, which] * factor + values[:, which] / (
                    points_at[which] - points_at[column]
                )
                values[:, which] = values[:, which] * factor
    return (values, slopes)


def basis_tables():
    lobatto = np.array([0.0, (1 - 5 ** (-0.5)) / 2, (1 + 5 ** (-0.5)) / 2, 1.0])
    gauss_open = np.array([(1 - 0.6**0.5) / 2, 0.5, (1 + 0.6**0.5) / 2])
    inner_pt = (3.0 / 7 - 2.0 / 7 * (6.0 / 5) ** 0.5) ** 0.5
    outer_pt = (3.0 / 7 + 2.0 / 7 * (6.0 / 5) ** 0.5) ** 0.5
    inner_wt = (18 + 30**0.5) / 36
    outer_wt = (18 - 30**0.5) / 36
    quad_points = (1 + np.array([-outer_pt, -inner_pt, inner_pt, outer_pt])) / 2
    quad_weight = np.array([outer_wt, inner_wt, inner_wt, outer_wt]) / 2
    closed, slopes = lagrange(lobatto, quad_points)
    opened, unused_slopes = lagrange(gauss_open, quad_points)
    return (closed, slopes, opened, quad_weight)


CLOSED, SLOPES, OPENED, WEIGHT = basis_tables()
DERIV = SLOPES @ np.linalg.inv(CLOSED)
OUTER, INNER = (0,), (1,)


def apply(table, given, parity, pairs=None):
    rows, columns = table.shape
    half = columns // 2
    sums = [given[c] + given[columns - 1 - c] for c in range(half)]
    diffs = [given[c] - given[columns - 1 - c] for c in range(half)]
    result = [None] * rows
    for q in pairs or range((rows + 1) // 2):
        even = None
        for c in range(half):
            term = sums[c] * float((table[q, c] + table[q, columns - 1 - c]) / 2)
            even = term if even is None else even + term
        if columns % 2:
            even = even + given[half] * float(table[q, half])
        if 2 * q + 1 == rows:
            result[q] = even
            continue
        odd = None
        for c in range(half):
            term = diffs[c] * float((table[q, c] - table[q, columns - 1 - c]) / 2)
            odd = term if odd is None else odd + term
        result[q] = even + odd
        result[rows - 1 - q] = even - odd if parity > 0 else odd - even
    return result


def along_rows(table, plane, parity=1, pairs=None):
    columns = [
        apply(table, [row[c] for row in plane], parity, pairs) for c in range(len(plane[0]))
    ]
    return [[column[q] for column in columns] for q in range(table.shape[0])]


def along_columns(table, plane, parity=1, pairs=None):
    return [apply(table, row, parity, pairs) for row in plane]


def combine(op, *planes):
    return [[op(*entries) for entries in zip(*rows)] for rows in zip(*planes)]


def plus(p, q):
    return combine(lambda s, t: s + t, p, q)


def minus(p, q):
    return combine(lambda s, t: s - t, p, q)


def times(p, q):
    return combine(lambda s, t: s * t, p, q)


def dof(comp, a, b, c):
    s = STRIDE[comp]
    return BASE[comp] + a * s[0] + b * s[1] + c * s[2]


def row_of(comp, a, b, c, element=0):
    return 8 * dof(comp, a, b, c) + element


def element(i, j, k):
    return 4 * k + 2 * i + j


def places(comp, axis):
    if comp == axis:
        return [(g, g // 3, g % 3) for g in range(6)]
    return [(g, 0, g) for g in range(4)] + [(g, 1, g - 3) for g in range(3, 7)]


def owners(comp, axis):
    last = 6 if comp == axis else 7
    return [(g, min(g // 3, 1), g - 3 * min(g // 3, 1)) for g in range(last)]


def prepare(flip, rel, con, flat, sign, mass, curl):
    for k in range(2):
        for i in range(2):
            at = pl.ds(4 * k + 2 * i, 2)
            flat[at, 0:DOFS] = 1.0 - 2.0 * flip[i][:, DOFS * k : DOFS * (k + 1)].astype(jnp.float32)
            flat[at, 256 : 256 + QPTS] = rel[i][:, QPTS * k : QPTS * (k + 1)]
            flat[at, 384 : 384 + QPTS] = con[i][:, QPTS * k : QPTS * (k + 1)]
    whole = flat[:, 0:DOFS]
    for d in range(DOFS):
        sign[d] = jnp.broadcast_to(whole[:, d : d + 1], (8, LANES))
    rel_all = flat[:, 256 : 256 + QPTS]
    con_all = flat[:, 384 : 384 + QPTS]
    for q in range(QPTS):
        weight = float(WEIGHT[q // 16] * WEIGHT[q // 4 % 4] * WEIGHT[q % 4])
        curl[q] = jnp.broadcast_to(rel_all[:, q : q + 1], (8, LANES)) * weight
        mass[q] = jnp.broadcast_to(con_all[:, q : q + 1], (8, LANES)) * weight


def quad(x, y, z):
    return 16 * x + 4 * y + z


def planes(ref, at):
    return [[ref[at(p, q)] for q in range(4)] for p in range(4)]


def put(ref, at, plane):
    for p, row in enumerate(plane):
        for q, value in enumerate(row):
            if value is not None:
                ref[at(p, q)] = value


def load_plane(dofs, sign, rows):
    return [
        [dofs[pl.ds(pl.multiple_of(8 * d, 8), 8), :] * sign[d] for d in row] for row in rows
    ]


def store_plane(dofs, sign, rows, plane):
    for row, values in zip(rows, plane):
        for d, value in zip(row, values):
            dofs[pl.ds(pl.multiple_of(8 * d, 8), 8), :] = value * sign[d]


def rows_fixed_b(comp, b):
    return [[dof(comp, a, b, c) for c in range(4 - (comp == 2))] for a in range(4 - (comp == 0))]


def rows_fixed_a(comp, a):
    return [[dof(comp, a, b, c) for c in range(4)] for b in range(3)]


def forward_y(dofs, sign, temp, u_y, c_x, c_z):
    @pl.loop(0, 4, unroll=True)
    def _(a):
        values = along_rows(OPENED, load_plane(dofs, sign, rows_fixed_a(1, a)))
        put(temp, lambda y, z: quad(a, y, z), along_columns(CLOSED, values))

    @pl.loop(0, 4, unroll=True)
    def _(y):
        at = lambda x, z: quad(x, y, z)
        u = along_rows(CLOSED, planes(temp, at))
        put(u_y, at, u)
        put(c_z, at, along_rows(DERIV, u, -1))
        put(c_x, at, along_columns(-DERIV, u, -1))


def start_x(dofs, sign, temp, b):
    values = along_rows(OPENED, load_plane(dofs, sign, rows_fixed_b(0, b)))
    put(temp, lambda x, z: quad(x, b, z), along_columns(CLOSED, values))


def start_z(dofs, sign, temp, b):
    values = along_columns(OPENED, load_plane(dofs, sign, rows_fixed_b(2, b)))
    put(temp, lambda x, z: quad(x, b, z), along_rows(CLOSED, values))


def forward_x(temp, curl, u_x, c_y, c_z):
    @pl.loop(0, 4, unroll=True)
    def _(x):
        at = lambda y, z: quad(x, y, z)
        u = along_rows(CLOSED, planes(temp, at))
        put(u_x, at, u)
        w_z = minus(planes(c_z, at), along_rows(DERIV, u, -1))
        put(c_z, at, times(planes(curl, at), w_z))
        put(c_y, at, along_columns(DERIV, u, -1))


def turn_z(temp, kept, mass, curl, c_x, c_y):
    @pl.loop(0, 4, unroll=True)
    def _(z):
        at = lambda x, y: quad(x, y, z)
        u = along_columns(CLOSED, planes(temp, at))
        scale = planes(curl, at)
        w_y = times(scale, minus(planes(c_y, at), along_rows(DERIV, u, -1)))
        w_x = times(scale, plus(planes(c_x, at), along_columns(DERIV, u, -1)))
        put(c_y, at, w_y)
        put(c_x, at, w_x)
        v = times(planes(mass, at), u)
        v = plus(v, along_columns(DERIV.T, w_x, -1))
        v = minus(v, along_rows(DERIV.T, w_y, -1))
        put(kept, at, v)
        put(temp, at, along_columns(CLOSED.T, v, 1, OUTER))


def inner_z(temp, kept):
    @pl.loop(0, 4, unroll=True)
    def _(z):
        at = lambda x, y: quad(x, y, z)
        put(temp, at, along_columns(CLOSED.T, planes(kept, at), 1, INNER))


def finish_z(dofs, sign, temp, first, last, step):
    @pl.loop(first, last, step=step, unroll=True)
    def _(b):
        values = along_rows(CLOSED.T, planes(temp, lambda x, z: quad(x, b, z)))
        store_plane(dofs, sign, rows_fixed_b(2, b), along_columns(OPENED.T, values))


def backward_x(mass, temp, kept, u_x, c_y, c_z):
    @pl.loop(0, 4, unroll=True)
    def _(x):
        at = lambda y, z: quad(x, y, z)
        v = times(planes(mass, at), planes(u_x, at))
        v = plus(v, along_columns(DERIV.T, planes(c_y, at), -1))
        v = minus(v, along_rows(DERIV.T, planes(c_z, at), -1))
        put(kept, at, v)
        put(temp, at, along_rows(CLOSED.T, v, 1, OUTER))


def inner_x(temp, kept):
    @pl.loop(0, 4, unroll=True)
    def _(x):
        at = lambda y, z: quad(x, y, z)
        put(temp, at, along_rows(CLOSED.T, planes(kept, at), 1, INNER))


def finish_x(dofs, sign, temp, first, last, step):
    @pl.loop(first, last, step=step, unroll=True)
    def _(b):
        values = along_columns(CLOSED.T, planes(temp, lambda x, z: quad(x, b, z)))
        store_plane(dofs, sign, rows_fixed_b(0, b), along_rows(OPENED.T, values))


def backward_y(dofs, sign, mass, temp, u_y, c_x, c_z):
    @pl.loop(0, 4, unroll=True)
    def _(y):
        at = lambda x, z: quad(x, y, z)
        v = times(planes(mass, at), planes(u_y, at))
        v = plus(v, along_rows(DERIV.T, planes(c_z, at), -1))
        v = minus(v, along_columns(DERIV.T, planes(c_x, at), -1))
        put(temp, at, along_rows(CLOSED.T, v))

    @pl.loop(0, 4, unroll=True)
    def _(a):
        values = along_columns(CLOSED.T, planes(temp, lambda y, z: quad(a, y, z)))
        store_plane(dofs, sign, rows_fixed_a(1, a), along_rows(OPENED.T, values))


def join_elements(dofs, comp, axes=(0, 1, 2), only_b=None):
    rows = lax.broadcasted_iota(jnp.int32, (8, LANES), 0)
    for axis, step in ((0, 2), (1, 1), (2, 4)):
        if comp == axis or axis not in axes:
            continue
        upper = (rows // step) % 2 == 1
        sizes = [range(3 if comp == other else 4) for other in range(3)]
        sizes[axis] = range(1)
        if only_b:
            sizes[1] = only_b
        for a in sizes[0]:
            for b in sizes[1]:
                for c in sizes[2]:
                    high = [a, b, c]
                    high[axis] = 3
                    to = pl.ds(row_of(comp, a, b, c), 8)
                    moved = pltpu.roll(dofs[pl.ds(row_of(comp, *high), 8), :], step, 0)
                    dofs[to, :] = dofs[to, :] + jnp.where(upper, moved, 0.0)


def scatter_own(vec, dofs):
    for comp in range(3):
        for x, i, a in places(comp, 0):
            for y, j, b in places(comp, 1):
                if x == 6 or y == 6:
                    continue
                for k in range(2):
                    count = 4 if comp != 2 and k == 0 else 3
                    at = row_of(comp, a, b, 0, element(i, j, k))
                    dofs[pl.ds(at, count, 8), :] = vec[comp, x, y, pl.ds(3 * k, count), :]


def scatter_line(dofs, comp, i, a, j, b, source):
    for k in range(2):
        count = 4 if comp != 2 and k == 0 else 3
        at = row_of(comp, a, b, 0, element(i, j, k))
        dofs[pl.ds(at, count, 8), :] = source(pl.ds(3 * k, count))


def scatter_xz_halo(dofs, r_x, r_z):
    for comp in (1, 2):
        for y, j, b in places(comp, 1):
            if y < 6:
                scatter_line(dofs, comp, 1, 3, j, b, lambda z: r_x[comp - 1, y, z, :])
    for x, i, a in places(0, 0):
        for j in range(2):
            count = 4 - j
            at = row_of(0, a, 0, 3, element(i, j, 1))
            dofs[pl.ds(at, count, 32), :] = r_z[0, x, pl.ds(3 * j, count), :]
    for x, i, a in places(1, 0):
        if x < 6:
            for j in range(2):
                at = row_of(1, a, 0, 3, element(i, j, 1))
                dofs[pl.ds(at, 3, 32), :] = r_z[1, x, pl.ds(3 * j, 3), :]


def scatter_xz_edge(dofs, r_e):
    for j in range(2):
        at = row_of(1, 3, 0, 3, element(1, j, 1))
        dofs[pl.ds(at, 3, 32), :] = r_e[1, pl.ds(3 * j, 3), :]


def scatter_y_halo(dofs, r_y, r_e):
    for comp in (0, 2):
        for x, i, a in places(comp, 0):
            if x < 6:
                scatter_line(dofs, comp, i, a, 1, 3, lambda z: r_y[comp // 2, x, z, :])
    for i in range(2):
        at = row_of(0, 0, 3, 3, element(i, 1, 1))
        dofs[pl.ds(at, 3, 128), :] = r_e[0, pl.ds(3 * i, 3), :]


def runs(comp, axis, fixed):
    local = [None if g is None else owners(comp, n)[g][1:] for n, g in enumerate(fixed)]
    result = []
    for half in range(2):
        count = 3 + half * (comp != axis)
        at = [(half, 0) if entry is None else entry for entry in local]
        (i, a), (j, b), (k, c) = at
        row = row_of(comp, a, b, c, element(i, j, k))
        result.append((pl.ds(3 * half, count), pl.ds(row, count, 8 * STRIDE[comp][axis])))
    return result


def owned(comp, axis):
    return range(6 if comp == axis else 7)


def to_grid(dofs, comp, out, line):
    other = 3 - line
    for x in owned(comp, 0):
        for q in owned(comp, other):
            fixed = [x, None, None]
            fixed[other] = q
            for grid, rows in runs(comp, line, fixed):
                out[x, q, grid, :] = dofs[rows, :]


def pack_face(dofs, comp, axis, line, pack):
    third = 3 - axis - line
    for side in range(2):
        for p in owned(comp, third):
            fixed = [None] * 3
            fixed[axis] = 6 * side
            fixed[third] = p
            for grid, rows in runs(comp, line, fixed):
                pack[side, p, grid, :] = dofs[rows, :]


def add_face(dofs, comp, axis, line, given):
    third = 3 - axis - line
    for side in range(2):
        for p in owned(comp, third):
            fixed = [None] * 3
            fixed[axis] = 6 * side
            fixed[third] = p
            for grid, rows in runs(comp, line, fixed):
                dofs[rows, :] = dofs[rows, :] + given[side, p, grid, :]


def edge_runs(comp, n):
    fixed = [None] * 3
    for axis, sign in zip(EDGE_AXES[comp], SIGNS[n]):
        fixed[axis] = 6 * (sign > 0)
    return runs(comp, comp, fixed)


def pack_edges(dofs, comp, edges):
    for n in range(4):
        for grid, rows in edge_runs(comp, n):
            edges[comp, n, grid, :] = dofs[rows, :]


def add_edges(dofs, comp, given):
    for n in range(4):
        for grid, rows in edge_runs(comp, n):
            dofs[rows, :] = dofs[rows, :] + given[comp, n, grid, :]


def kernel(
    sizes,
    vec_hbm,
    flip_hbm,
    rel_hbm,
    con_hbm,
    out_x,
    out_y,
    out_z,
    vec,
    flip,
    rel,
    con,
    flat,
    sign,
    mass,
    curl,
    dofs,
    temp,
    u_x,
    u_y,
    c_x,
    c_y,
    c_z,
    s_z,
    s_e,
    r_x,
    r_y,
    r_z,
    r_e,
    t_x,
    t_z,
    v_x,
    v_z,
    p_xy,
    p_xz,
    p_yx,
    p_yz,
    p_zx,
    p_zy,
    p_e,
    f_xy,
    f_xz,
    f_yx,
    f_yz,
    f_zx,
    f_zy,
    f_e,
    load_sem,
    send_sem,
    recv_sem,
):
    me = [lax.axis_index(axis) for axis in AXES]

    def neighbour(*steps):
        return tuple(lax.rem(me[n] + steps[n] + sizes[n], sizes[n]) for n in range(3))

    loads = [
        pltpu.make_async_copy(source, target, load_sem.at[n])
        for n, (source, target) in enumerate(
            ((vec_hbm, vec), (flip_hbm, flip), (rel_hbm, rel), (con_hbm, con))
        )
    ]
    for copy in loads:
        copy.start()

    barrier = pltpu.get_barrier_semaphore()
    upper = ((0, 1, 0), (1, 1, 0), (0, 1, 1), (1, 0, 0), (1, 0, 1), (0, 0, 1))
    for steps in upper:
        pl.semaphore_signal(barrier, inc=1, device_id=neighbour(*steps), device_id_type=MESH)

    copies = []

    def send(source, target, *steps):
        n = len(copies)
        copy = pltpu.make_async_remote_copy(
            src_ref=source,
            dst_ref=target,
            send_sem=send_sem.at[n],
            recv_sem=recv_sem.at[n],
            device_id=neighbour(*steps),
            device_id_type=MESH,
        )
        copy.start()
        copies.append(copy)
        return copy

    def send_faces(axis, pack, target):
        faces = []
        for side in range(2):
            steps = [(2 * side - 1) * (axis == n) for n in range(3)]
            faces.append(send(pack.at[side], target.at[1 - side], *steps))
        return faces

    def send_edges(comp):
        sent = []
        for n, pair in enumerate(SIGNS):
            steps = [0, 0, 0]
            for axis, step in zip(EDGE_AXES[comp], pair):
                steps[axis] = step
            sent.append(send(p_e.at[comp, n], f_e.at[comp, 3 - n], *steps))
        return sent

    def receive(arriving):
        for copy in arriving:
            copy.wait_recv()

    loads[0].wait()
    for comp in range(2):
        for x in range(6):
            for y in range(6):
                s_z[comp, x, pl.ds(y, 1), :] = vec[comp, x, y, pl.ds(0, 1), :]
    for n in range(6):
        s_e[0, pl.ds(n, 1), :] = vec[0, n, 0, pl.ds(0, 1), :]
        s_e[1, pl.ds(n, 1), :] = vec[1, 0, n, pl.ds(0, 1), :]
    pl.semaphore_wait(barrier, len(upper))
    xy_halo = [send(vec.at[2, 0, 0], r_e.at[2], -1, -1, 0)]
    y_halo = [
        send(s_e.at[0], r_e.at[0], 0, -1, -1),
        send(vec.at[0, :, 0], r_y.at[0], 0, -1, 0),
        send(vec.at[2, :, 0], r_y.at[1], 0, -1, 0),
    ]
    xz_halo = [
        send(s_e.at[1], r_e.at[1], -1, 0, -1),
        send(vec.at[pl.ds(1, 2), 0], r_x, -1, 0, 0),
        send(s_z, r_z, 0, 0, -1),
    ]

    scatter_own(vec, dofs)
    for copy in loads[1:]:
        copy.wait()
    prepare(flip, rel, con, flat, sign, mass, curl)
    receive(xz_halo[1:])
    scatter_xz_halo(dofs, r_x, r_z)

    @pl.loop(0, 3, unroll=1)
    def _(b):
        start_x(dofs, sign, t_x, b)
        start_z(dofs, sign, t_z, b)

    receive(xz_halo[:1])
    scatter_xz_edge(dofs, r_e)
    forward_y(dofs, sign, temp, u_y, c_x, c_z)
    receive(y_halo)
    scatter_y_halo(dofs, r_y, r_e)
    start_x(dofs, sign, t_x, 3)
    forward_x(t_x, curl, u_x, c_y, c_z)
    receive(xy_halo)
    scatter_line(dofs, 2, 1, 3, 1, 3, lambda z: r_e[2, z, :])
    start_z(dofs, sign, t_z, 3)
    turn_z(t_z, v_z, mass, curl, c_x, c_y)
    finish_z(dofs, sign, t_z, 0, 4, 3)
    join_elements(dofs, 2, (0,), (0, 3))
    pack_edges(dofs, 2, p_e)
    edges_z = send_edges(2)
    pack_face(dofs, 2, 1, 2, p_yz)
    faces_yz = send_faces(1, p_yz, f_yz)

    backward_x(mass, t_x, v_x, u_x, c_y, c_z)
    finish_x(dofs, sign, t_x, 0, 4, 3)
    join_elements(dofs, 0, (2,), (0, 3))
    pack_edges(dofs, 0, p_e)
    edges_x = send_edges(0)
    pack_face(dofs, 0, 1, 2, p_yx)
    faces_yx = send_faces(1, p_yx, f_yx)

    backward_y(dofs, sign, mass, temp, u_y, c_x, c_z)
    join_elements(dofs, 1)
    pack_edges(dofs, 1, p_e)
    edges_y = send_edges(1)
    pack_face(dofs, 1, 0, 2, p_xy)
    faces_xy = send_faces(0, p_xy, f_xy)

    inner_z(t_z, v_z)
    finish_z(dofs, sign, t_z, 1, 3, 1)
    join_elements(dofs, 2, (0,), (1, 2))
    join_elements(dofs, 2, (1,))
    pack_face(dofs, 2, 0, 1, p_xz)
    faces_xz = send_faces(0, p_xz, f_xz)
    pack_face(dofs, 1, 2, 1, p_zy)
    faces_zy = send_faces(2, p_zy, f_zy)
    inner_x(t_x, v_x)
    finish_x(dofs, sign, t_x, 1, 3, 1)
    join_elements(dofs, 0, (2,), (1, 2))
    join_elements(dofs, 0, (1,))
    pack_face(dofs, 0, 2, 1, p_zx)
    faces_zx = send_faces(2, p_zx, f_zx)

    receive(faces_zy + edges_y)
    add_face(dofs, 1, 2, 1, f_zy)
    add_edges(dofs, 1, f_e)
    to_grid(dofs, 1, out_y, 2)
    receive(faces_xy)
    for side in range(2):
        out_y[6 * side] = out_y[6 * side] + f_xy[side]
    receive(faces_zx)
    add_face(dofs, 0, 2, 1, f_zx)
    to_grid(dofs, 0, out_x, 2)
    receive(faces_yz + edges_z)
    add_face(dofs, 2, 1, 2, f_yz)
    add_edges(dofs, 2, f_e)
    to_grid(dofs, 2, out_z, 1)
    receive(faces_xz)
    for side in range(2):
        out_z[6 * side] = out_z[6 * side] + f_xz[side]
    receive(edges_x)
    for n, pair in enumerate(SIGNS):
        y, z = 6 * (pair[0] > 0), 6 * (pair[1] > 0)
        for x in range(6):
            at = pl.ds(z, 1)
            out_x[x, y, at, :] = out_x[x, y, at, :] + f_e[0, n, pl.ds(x, 1), :]
    receive(faces_yx)
    for side in range(2):
        for x in range(6):
            out_x[x, 6 * side] = out_x[x, 6 * side] + f_yx[side, x]
    for copy in copies:
        copy.wait_send()


def put_out(in_x, in_y, in_z, out_x, out_y, out_z, sem):
    pairs = ((in_x, out_x), (in_y, out_y), (in_z, out_z))
    copies = [pltpu.make_async_copy(*pair, sem.at[n]) for n, pair in enumerate(pairs)]
    for copy in copies:
        copy.start()
    for copy in copies:
        copy.wait()


def on_device(sizes, vectors, orient_flip, reluctivity, conductivity):
    f32 = jnp.float32
    regs = lambda n: pltpu.VMEM((n, 8, LANES), f32)
    grid = ((6, 7, 7, LANES), (7, 6, 7, LANES), (7, 6, 7, LANES))
    faces = [
        pltpu.VMEM(shape, f32)
        for shape in (
            (2, 6, 7, LANES),
            (2, 6, 7, LANES),
            (2, 6, 7, LANES),
            (2, 7, 6, LANES),
            (2, 6, 7, LANES),
            (2, 7, 6, LANES),
            (3, 4, 6, LANES),
        )
    ]
    results = pl.pallas_call(
        lambda *refs: kernel(sizes, *refs),
        out_shape=[pltpu.VMEM(shape, f32) for shape in grid],
        in_specs=[pl.BlockSpec(memory_space=pl.ANY)] * 4,
        out_specs=[pl.BlockSpec(memory_space=pltpu.VMEM)] * 3,
        scratch_shapes=[
            pltpu.VMEM((3, 6, 6, 6, LANES), f32),
            pltpu.VMEM(orient_flip.shape, jnp.int32),
            pltpu.VMEM(reluctivity.shape, f32),
            pltpu.VMEM(conductivity.shape, f32),
            pltpu.VMEM((8, 512), f32),
            regs(DOFS),
            regs(QPTS),
            regs(QPTS),
            pltpu.VMEM((8 * DOFS, LANES), f32),
            regs(QPTS),
            regs(QPTS),
            regs(QPTS),
            regs(QPTS),
            regs(QPTS),
            regs(QPTS),
            pltpu.VMEM((2, 6, 6, LANES), f32),
            pltpu.VMEM((2, 6, LANES), f32),
            pltpu.VMEM((2, 6, 6, LANES), f32),
            pltpu.VMEM((2, 6, 6, LANES), f32),
            pltpu.VMEM((2, 6, 6, LANES), f32),
            pltpu.VMEM((3, 6, LANES), f32),
            *[regs(QPTS)] * 4,
            *faces,
            *faces,
            pltpu.SemaphoreType.DMA((4,)),
            pltpu.SemaphoreType.DMA((31,)),
            pltpu.SemaphoreType.DMA((31,)),
        ],
        compiler_params=pltpu.CompilerParams(collective_id=0, has_side_effects=True),
        name="curlcurl",
    )(vectors, orient_flip, reluctivity, conductivity)
    results = [pltpu.with_memory_space_constraint(result, pltpu.VMEM) for result in results]
    out_x, out_y, out_z = pl.pallas_call(
        put_out,
        out_shape=[jax.ShapeDtypeStruct(shape, f32) for shape in grid],
        in_specs=[pl.BlockSpec(memory_space=pltpu.VMEM)] * 3,
        out_specs=[pl.BlockSpec(memory_space=pl.ANY)] * 3,
        scratch_shapes=[pltpu.SemaphoreType.DMA((3,))],
        name="putout",
    )(*results)
    return (out_x, out_y, jnp.swapaxes(out_z, 1, 2))


def solution(mesh):
    sizes = tuple(mesh.shape[axis] for axis in AXES)
    return jax.shard_map(
        lambda *args: on_device(sizes, *args),
        mesh=mesh,
        in_specs=(
            P(None, "gx", "gy", "gz", None),
            P("gx", "gy", "gz"),
            P("gx", "gy", "gz"),
            P("gx", "gy", "gz"),
        ),
        out_specs=(P("gx", "gy", "gz", None), P("gx", "gy", "gz", None), P("gx", "gy", "gz", None)),
        check_vma=False,
    )
```

```python
import jax
import jax.numpy as jnp
import numpy as np
from jax import lax
from jax.experimental import pallas as pl
from jax.experimental.pallas import tpu as pltpu
from jax.sharding import PartitionSpec as P

MESH = pl.DeviceIdType.MESH
AXES = ("gx", "gy", "gz")
LANES = 128
DOFS = 144
QPTS = 64
BASE = (0, 48, 96)
STRIDE = ((16, 4, 1), (12, 4, 1), (12, 3, 1))
EDGE_AXES = ((1, 2), (0, 2), (0, 1))
SIGNS = ((-1, -1), (-1, 1), (1, -1), (1, 1))


def lagrange(points_at, evaluate_at):
    amount = len(points_at)
    values = np.ones((len(evaluate_at), amount))
    slopes = np.zeros((len(evaluate_at), amount))
    for which in range(amount):
        for column in range(amount):
            if column != which:
                factor = (evaluate_at - points_at[column]) / (points_at[which] - points_at[column])
                slopes[:, which] = slopes[:, which] * factor + values[:, which] / (
                    points_at[which] - points_at[column]
                )
                values[:, which] = values[:, which] * factor
    return (values, slopes)


def basis_tables():
    lobatto = np.array([0.0, (1 - 5 ** (-0.5)) / 2, (1 + 5 ** (-0.5)) / 2, 1.0])
    gauss_open = np.array([(1 - 0.6**0.5) / 2, 0.5, (1 + 0.6**0.5) / 2])
    inner_pt = (3.0 / 7 - 2.0 / 7 * (6.0 / 5) ** 0.5) ** 0.5
    outer_pt = (3.0 / 7 + 2.0 / 7 * (6.0 / 5) ** 0.5) ** 0.5
    inner_wt = (18 + 30**0.5) / 36
    outer_wt = (18 - 30**0.5) / 36
    quad_points = (1 + np.array([-outer_pt, -inner_pt, inner_pt, outer_pt])) / 2
    quad_weight = np.array([outer_wt, inner_wt, inner_wt, outer_wt]) / 2
    closed, slopes = lagrange(lobatto, quad_points)
    opened, unused_slopes = lagrange(gauss_open, quad_points)
    return (closed, slopes, opened, quad_weight)


CLOSED, SLOPES, OPENED, WEIGHT = basis_tables()
DERIV = SLOPES @ np.linalg.inv(CLOSED)
OUTER, INNER = (0,), (1,)


def apply(table, given, parity, pairs=None):
    rows, columns = table.shape
    half = columns // 2
    sums = [given[c] + given[columns - 1 - c] for c in range(half)]
    diffs = [given[c] - given[columns - 1 - c] for c in range(half)]
    result = [None] * rows
    for q in pairs or range((rows + 1) // 2):
        even = None
        for c in range(half):
            term = sums[c] * float((table[q, c] + table[q, columns - 1 - c]) / 2)
            even = term if even is None else even + term
        if columns % 2:
            even = even + given[half] * float(table[q, half])
        if 2 * q + 1 == rows:
            result[q] = even
            continue
        odd = None
        for c in range(half):
            term = diffs[c] * float((table[q, c] - table[q, columns - 1 - c]) / 2)
            odd = term if odd is None else odd + term
        result[q] = even + odd
        result[rows - 1 - q] = even - odd if parity > 0 else odd - even
    return result


def along_rows(table, plane, parity=1, pairs=None):
    columns = [
        apply(table, [row[c] for row in plane], parity, pairs) for c in range(len(plane[0]))
    ]
    return [[column[q] for column in columns] for q in range(table.shape[0])]


def along_columns(table, plane, parity=1, pairs=None):
    return [apply(table, row, parity, pairs) for row in plane]


def combine(op, *planes):
    return [[op(*entries) for entries in zip(*rows)] for rows in zip(*planes)]


def plus(p, q):
    return combine(lambda s, t: s + t, p, q)


def minus(p, q):
    return combine(lambda s, t: s - t, p, q)


def times(p, q):
    return combine(lambda s, t: s * t, p, q)


def dof(comp, a, b, c):
    s = STRIDE[comp]
    return BASE[comp] + a * s[0] + b * s[1] + c * s[2]


def row_of(comp, a, b, c, element=0):
    return 8 * dof(comp, a, b, c) + element


def element(i, j, k):
    return 4 * k + 2 * i + j


def places(comp, axis):
    if comp == axis:
        return [(g, g // 3, g % 3) for g in range(6)]
    return [(g, 0, g) for g in range(4)] + [(g, 1, g - 3) for g in range(3, 7)]


def owners(comp, axis):
    last = 6 if comp == axis else 7
    return [(g, min(g // 3, 1), g - 3 * min(g // 3, 1)) for g in range(last)]


def prepare(flip, rel, con, flat, sign, mass, curl):
    for k in range(2):
        for i in range(2):
            at = pl.ds(4 * k + 2 * i, 2)
            flat[at, 0:DOFS] = 1.0 - 2.0 * flip[i][:, DOFS * k : DOFS * (k + 1)].astype(jnp.float32)
            flat[at, 256 : 256 + QPTS] = rel[i][:, QPTS * k : QPTS * (k + 1)]
            flat[at, 384 : 384 + QPTS] = con[i][:, QPTS * k : QPTS * (k + 1)]
    whole = flat[:, 0:DOFS]
    for d in range(DOFS):
        sign[d] = jnp.broadcast_to(whole[:, d : d + 1], (8, LANES))
    rel_all = flat[:, 256 : 256 + QPTS]
    con_all = flat[:, 384 : 384 + QPTS]
    for q in range(QPTS):
        weight = float(WEIGHT[q // 16] * WEIGHT[q // 4 % 4] * WEIGHT[q % 4])
        curl[q] = jnp.broadcast_to(rel_all[:, q : q + 1], (8, LANES)) * weight
        mass[q] = jnp.broadcast_to(con_all[:, q : q + 1], (8, LANES)) * weight


def quad(x, y, z):
    return 16 * x + 4 * y + z


def planes(ref, at):
    return [[ref[at(p, q)] for q in range(4)] for p in range(4)]


def put(ref, at, plane):
    for p, row in enumerate(plane):
        for q, value in enumerate(row):
            if value is not None:
                ref[at(p, q)] = value


def load_plane(dofs, sign, rows):
    return [
        [dofs[pl.ds(pl.multiple_of(8 * d, 8), 8), :] * sign[d] for d in row] for row in rows
    ]


def store_plane(dofs, sign, rows, plane):
    for row, values in zip(rows, plane):
        for d, value in zip(row, values):
            dofs[pl.ds(pl.multiple_of(8 * d, 8), 8), :] = value * sign[d]


def rows_fixed_b(comp, b):
    return [[dof(comp, a, b, c) for c in range(4 - (comp == 2))] for a in range(4 - (comp == 0))]


def rows_fixed_a(comp, a):
    return [[dof(comp, a, b, c) for c in range(4)] for b in range(3)]


def forward_y(dofs, sign, temp, u_y, c_x, c_z):
    @pl.loop(0, 4, unroll=True)
    def _(a):
        values = along_rows(OPENED, load_plane(dofs, sign, rows_fixed_a(1, a)))
        put(temp, lambda y, z: quad(a, y, z), along_columns(CLOSED, values))

    @pl.loop(0, 4, unroll=True)
    def _(y):
        at = lambda x, z: quad(x, y, z)
        u = along_rows(CLOSED, planes(temp, at))
        put(u_y, at, u)
        put(c_z, at, along_rows(DERIV, u, -1))
        put(c_x, at, along_columns(-DERIV, u, -1))


def start_x(dofs, sign, temp, b):
    values = along_rows(OPENED, load_plane(dofs, sign, rows_fixed_b(0, b)))
    put(temp, lambda x, z: quad(x, b, z), along_columns(CLOSED, values))


def start_z(dofs, sign, temp, b):
    values = along_columns(OPENED, load_plane(dofs, sign, rows_fixed_b(2, b)))
    put(temp, lambda x, z: quad(x, b, z), along_rows(CLOSED, values))


def forward_x(temp, curl, u_x, c_y, c_z):
    @pl.loop(0, 4, unroll=True)
    def _(x):
        at = lambda y, z: quad(x, y, z)
        u = along_rows(CLOSED, planes(temp, at))
        put(u_x, at, u)
        w_z = minus(planes(c_z, at), along_rows(DERIV, u, -1))
        put(c_z, at, times(planes(curl, at), w_z))
        put(c_y, at, along_columns(DERIV, u, -1))


def turn_z(temp, kept, mass, curl, c_x, c_y):
    @pl.loop(0, 4, unroll=True)
    def _(z):
        at = lambda x, y: quad(x, y, z)
        u = along_columns(CLOSED, planes(temp, at))
        scale = planes(curl, at)
        w_y = times(scale, minus(planes(c_y, at), along_rows(DERIV, u, -1)))
        w_x = times(scale, plus(planes(c_x, at), along_columns(DERIV, u, -1)))
        put(c_y, at, w_y)
        put(c_x, at, w_x)
        v = times(planes(mass, at), u)
        v = plus(v, along_columns(DERIV.T, w_x, -1))
        v = minus(v, along_rows(DERIV.T, w_y, -1))
        put(kept, at, v)
        put(temp, at, along_columns(CLOSED.T, v, 1, OUTER))


def inner_z(temp, kept):
    @pl.loop(0, 4, unroll=True)
    def _(z):
        at = lambda x, y: quad(x, y, z)
        put(temp, at, along_columns(CLOSED.T, planes(kept, at), 1, INNER))


def finish_z(dofs, sign, temp, first, last, step):
    @pl.loop(first, last, step=step, unroll=True)
    def _(b):
        values = along_rows(CLOSED.T, planes(temp, lambda x, z: quad(x, b, z)))
        store_plane(dofs, sign, rows_fixed_b(2, b), along_columns(OPENED.T, values))


def backward_x(mass, temp, kept, u_x, c_y, c_z):
    @pl.loop(0, 4, unroll=True)
    def _(x):
        at = lambda y, z: quad(x, y, z)
        v = times(planes(mass, at), planes(u_x, at))
        v = plus(v, along_columns(DERIV.T, planes(c_y, at), -1))
        v = minus(v, along_rows(DERIV.T, planes(c_z, at), -1))
        put(kept, at, v)
        put(temp, at, along_rows(CLOSED.T, v, 1, OUTER))


def inner_x(temp, kept):
    @pl.loop(0, 4, unroll=True)
    def _(x):
        at = lambda y, z: quad(x, y, z)
        put(temp, at, along_rows(CLOSED.T, planes(kept, at), 1, INNER))


def finish_x(dofs, sign, temp, first, last, step):
    @pl.loop(first, last, step=step, unroll=True)
    def _(b):
        values = along_columns(CLOSED.T, planes(temp, lambda x, z: quad(x, b, z)))
        store_plane(dofs, sign, rows_fixed_b(0, b), along_rows(OPENED.T, values))


def backward_y(dofs, sign, mass, temp, u_y, c_x, c_z):
    @pl.loop(0, 4, unroll=True)
    def _(y):
        at = lambda x, z: quad(x, y, z)
        v = times(planes(mass, at), planes(u_y, at))
        v = plus(v, along_rows(DERIV.T, planes(c_z, at), -1))
        v = minus(v, along_columns(DERIV.T, planes(c_x, at), -1))
        put(temp, at, along_rows(CLOSED.T, v))

    @pl.loop(0, 4, unroll=True)
    def _(a):
        values = along_columns(CLOSED.T, planes(temp, lambda y, z: quad(a, y, z)))
        store_plane(dofs, sign, rows_fixed_a(1, a), along_rows(OPENED.T, values))


def join_elements(dofs, comp, axes=(0, 1, 2), only_b=None):
    rows = lax.broadcasted_iota(jnp.int32, (8, LANES), 0)
    for axis, step in ((0, 2), (1, 1), (2, 4)):
        if comp == axis or axis not in axes:
            continue
        upper = (rows // step) % 2 == 1
        sizes = [range(3 if comp == other else 4) for other in range(3)]
        sizes[axis] = range(1)
        if only_b:
            sizes[1] = only_b
        for a in sizes[0]:
            for b in sizes[1]:
                for c in sizes[2]:
                    high = [a, b, c]
                    high[axis] = 3
                    to = pl.ds(row_of(comp, a, b, c), 8)
                    moved = pltpu.roll(dofs[pl.ds(row_of(comp, *high), 8), :], step, 0)
                    dofs[to, :] = dofs[to, :] + jnp.where(upper, moved, 0.0)


def scatter_own(vec, dofs):
    for comp in range(3):
        for x, i, a in places(comp, 0):
            for y, j, b in places(comp, 1):
                if x == 6 or y == 6:
                    continue
                for k in range(2):
                    count = 4 if comp != 2 and k == 0 else 3
                    at = row_of(comp, a, b, 0, element(i, j, k))
                    dofs[pl.ds(at, count, 8), :] = vec[comp, x, y, pl.ds(3 * k, count), :]


def scatter_line(dofs, comp, i, a, j, b, source):
    for k in range(2):
        count = 4 if comp != 2 and k == 0 else 3
        at = row_of(comp, a, b, 0, element(i, j, k))
        dofs[pl.ds(at, count, 8), :] = source(pl.ds(3 * k, count))


def scatter_xz_halo(dofs, r_x, r_z):
    for comp in (1, 2):
        for y, j, b in places(comp, 1):
            if y < 6:
                scatter_line(dofs, comp, 1, 3, j, b, lambda z: r_x[comp - 1, y, z, :])
    for x, i, a in places(0, 0):
        for j in range(2):
            count = 4 - j
            at = row_of(0, a, 0, 3, element(i, j, 1))
            dofs[pl.ds(at, count, 32), :] = r_z[0, x, pl.ds(3 * j, count), :]
    for x, i, a in places(1, 0):
        if x < 6:
            for j in range(2):
                at = row_of(1, a, 0, 3, element(i, j, 1))
                dofs[pl.ds(at, 3, 32), :] = r_z[1, x, pl.ds(3 * j, 3), :]


def scatter_xz_edge(dofs, r_e):
    for j in range(2):
        at = row_of(1, 3, 0, 3, element(1, j, 1))
        dofs[pl.ds(at, 3, 32), :] = r_e[1, pl.ds(3 * j, 3), :]


def scatter_y_halo(dofs, r_y, r_e):
    for comp in (0, 2):
        for x, i, a in places(comp, 0):
            if x < 6:
                scatter_line(dofs, comp, i, a, 1, 3, lambda z: r_y[comp // 2, x, z, :])
    for i in range(2):
        at = row_of(0, 0, 3, 3, element(i, 1, 1))
        dofs[pl.ds(at, 3, 128), :] = r_e[0, pl.ds(3 * i, 3), :]


def runs(comp, axis, fixed):
    local = [None if g is None else owners(comp, n)[g][1:] for n, g in enumerate(fixed)]
    result = []
    for half in range(2):
        count = 3 + half * (comp != axis)
        at = [(half, 0) if entry is None else entry for entry in local]
        (i, a), (j, b), (k, c) = at
        row = row_of(comp, a, b, c, element(i, j, k))
        result.append((pl.ds(3 * half, count), pl.ds(row, count, 8 * STRIDE[comp][axis])))
    return result


def owned(comp, axis):
    return range(6 if comp == axis else 7)


def to_grid(dofs, comp, out, line):
    other = 3 - line
    for x in owned(comp, 0):
        for q in owned(comp, other):
            fixed = [x, None, None]
            fixed[other] = q
            for grid, rows in runs(comp, line, fixed):
                out[x, q, grid, :] = dofs[rows, :]


def pack_face(dofs, comp, axis, line, pack):
    third = 3 - axis - line
    for side in range(2):
        for p in owned(comp, third):
            fixed = [None] * 3
            fixed[axis] = 6 * side
            fixed[third] = p
            for grid, rows in runs(comp, line, fixed):
                pack[side, p, grid, :] = dofs[rows, :]


def add_face(dofs, comp, axis, line, given):
    third = 3 - axis - line
    for side in range(2):
        for p in owned(comp, third):
            fixed = [None] * 3
            fixed[axis] = 6 * side
            fixed[third] = p
            for grid, rows in runs(comp, line, fixed):
                dofs[rows, :] = dofs[rows, :] + given[side, p, grid, :]


def edge_runs(comp, n):
    fixed = [None] * 3
    for axis, sign in zip(EDGE_AXES[comp], SIGNS[n]):
        fixed[axis] = 6 * (sign > 0)
    return runs(comp, comp, fixed)


def pack_edges(dofs, comp, edges):
    for n in range(4):
        for grid, rows in edge_runs(comp, n):
            edges[comp, n, grid, :] = dofs[rows, :]


def add_edges(dofs, comp, given):
    for n in range(4):
        for grid, rows in edge_runs(comp, n):
            dofs[rows, :] = dofs[rows, :] + given[comp, n, grid, :]


def kernel(
    sizes,
    vec_hbm,
    flip_hbm,
    rel_hbm,
    con_hbm,
    out_x,
    out_y,
    out_z,
    vec,
    flip,
    rel,
    con,
    flat,
    sign,
    mass,
    curl,
    dofs,
    temp,
    u_x,
    u_y,
    c_x,
    c_y,
    c_z,
    s_z,
    s_e,
    r_x,
    r_y,
    r_z,
    r_e,
    t_x,
    t_z,
    v_x,
    v_z,
    p_xy,
    p_xz,
    p_yx,
    p_yz,
    p_zx,
    p_zy,
    p_e,
    f_xy,
    f_xz,
    f_yx,
    f_yz,
    f_zx,
    f_zy,
    f_e,
    load_sem,
    send_sem,
    recv_sem,
):
    me = [lax.axis_index(axis) for axis in AXES]

    def neighbour(*steps):
        return tuple(lax.rem(me[n] + steps[n] + sizes[n], sizes[n]) for n in range(3))

    loads = [
        pltpu.make_async_copy(source, target, load_sem.at[n])
        for n, (source, target) in enumerate(
            ((vec_hbm, vec), (flip_hbm, flip), (rel_hbm, rel), (con_hbm, con))
        )
    ]
    for copy in loads:
        copy.start()

    barrier = pltpu.get_barrier_semaphore()
    upper = ((0, 1, 0), (1, 1, 0), (0, 1, 1), (1, 0, 0), (1, 0, 1), (0, 0, 1))
    for steps in upper:
        pl.semaphore_signal(barrier, inc=1, device_id=neighbour(*steps), device_id_type=MESH)

    copies = []

    def send(source, target, *steps):
        n = len(copies)
        copy = pltpu.make_async_remote_copy(
            src_ref=source,
            dst_ref=target,
            send_sem=send_sem.at[n],
            recv_sem=recv_sem.at[n],
            device_id=neighbour(*steps),
            device_id_type=MESH,
        )
        copy.start()
        copies.append(copy)
        return copy

    def send_faces(axis, pack, target):
        faces = []
        for side in range(2):
            steps = [(2 * side - 1) * (axis == n) for n in range(3)]
            faces.append(send(pack.at[side], target.at[1 - side], *steps))
        return faces

    def send_edges(comp):
        sent = []
        for n, pair in enumerate(SIGNS):
            steps = [0, 0, 0]
            for axis, step in zip(EDGE_AXES[comp], pair):
                steps[axis] = step
            sent.append(send(p_e.at[comp, n], f_e.at[comp, 3 - n], *steps))
        return sent

    def receive(arriving):
        for copy in arriving:
            copy.wait_recv()

    loads[0].wait()
    for comp in range(2):
        for x in range(6):
            for y in range(6):
                s_z[comp, x, pl.ds(y, 1), :] = vec[comp, x, y, pl.ds(0, 1), :]
    for n in range(6):
        s_e[0, pl.ds(n, 1), :] = vec[0, n, 0, pl.ds(0, 1), :]
        s_e[1, pl.ds(n, 1), :] = vec[1, 0, n, pl.ds(0, 1), :]
    scatter_own(vec, dofs)
    pl.semaphore_wait(barrier, len(upper))
    xy_halo = [send(vec.at[2, 0, 0], r_e.at[2], -1, -1, 0)]
    y_halo = [
        send(s_e.at[0], r_e.at[0], 0, -1, -1),
        send(vec.at[0, :, 0], r_y.at[0], 0, -1, 0),
        send(vec.at[2, :, 0], r_y.at[1], 0, -1, 0),
    ]
    xz_halo = [
        send(s_e.at[1], r_e.at[1], -1, 0, -1),
        send(vec.at[pl.ds(1, 2), 0], r_x, -1, 0, 0),
        send(s_z, r_z, 0, 0, -1),
    ]

    for copy in loads[1:]:
        copy.wait()
    prepare(flip, rel, con, flat, sign, mass, curl)
    receive(xz_halo[1:])
    scatter_xz_halo(dofs, r_x, r_z)

    @pl.loop(0, 3, unroll=1)
    def _(b):
        start_x(dofs, sign, t_x, b)
        start_z(dofs, sign, t_z, b)

    receive(xz_halo[:1])
    scatter_xz_edge(dofs, r_e)
    forward_y(dofs, sign, temp, u_y, c_x, c_z)
    receive(y_halo)
    scatter_y_halo(dofs, r_y, r_e)
    start_x(dofs, sign, t_x, 3)
    forward_x(t_x, curl, u_x, c_y, c_z)
    receive(xy_halo)
    scatter_line(dofs, 2, 1, 3, 1, 3, lambda z: r_e[2, z, :])
    start_z(dofs, sign, t_z, 3)
    turn_z(t_z, v_z, mass, curl, c_x, c_y)
    finish_z(dofs, sign, t_z, 0, 4, 3)
    join_elements(dofs, 2, (0,), (0, 3))
    pack_edges(dofs, 2, p_e)
    edges_z = send_edges(2)
    pack_face(dofs, 2, 1, 2, p_yz)
    faces_yz = send_faces(1, p_yz, f_yz)

    backward_y(dofs, sign, mass, temp, u_y, c_x, c_z)
    join_elements(dofs, 1)
    pack_edges(dofs, 1, p_e)
    edges_y = send_edges(1)
    pack_face(dofs, 1, 0, 2, p_xy)
    faces_xy = send_faces(0, p_xy, f_xy)

    backward_x(mass, t_x, v_x, u_x, c_y, c_z)
    finish_x(dofs, sign, t_x, 0, 4, 3)
    join_elements(dofs, 0, (2,), (0, 3))
    pack_edges(dofs, 0, p_e)
    edges_x = send_edges(0)
    pack_face(dofs, 0, 1, 2, p_yx)
    faces_yx = send_faces(1, p_yx, f_yx)

    inner_z(t_z, v_z)
    finish_z(dofs, sign, t_z, 1, 3, 1)
    join_elements(dofs, 2, (0,), (1, 2))
    join_elements(dofs, 2, (1,))
    pack_face(dofs, 2, 0, 1, p_xz)
    faces_xz = send_faces(0, p_xz, f_xz)
    pack_face(dofs, 1, 2, 1, p_zy)
    faces_zy = send_faces(2, p_zy, f_zy)
    inner_x(t_x, v_x)
    finish_x(dofs, sign, t_x, 1, 3, 1)
    join_elements(dofs, 0, (2,), (1, 2))
    join_elements(dofs, 0, (1,))
    pack_face(dofs, 0, 2, 1, p_zx)
    faces_zx = send_faces(2, p_zx, f_zx)

    receive(faces_zy + edges_y)
    add_face(dofs, 1, 2, 1, f_zy)
    add_edges(dofs, 1, f_e)
    to_grid(dofs, 1, out_y, 2)
    receive(faces_xy)
    for side in range(2):
        out_y[6 * side] = out_y[6 * side] + f_xy[side]
    receive(faces_zx)
    add_face(dofs, 0, 2, 1, f_zx)
    to_grid(dofs, 0, out_x, 2)
    receive(faces_yz + edges_z)
    add_face(dofs, 2, 1, 2, f_yz)
    add_edges(dofs, 2, f_e)
    to_grid(dofs, 2, out_z, 1)
    receive(faces_xz)
    for side in range(2):
        out_z[6 * side] = out_z[6 * side] + f_xz[side]
    receive(edges_x)
    for n, pair in enumerate(SIGNS):
        y, z = 6 * (pair[0] > 0), 6 * (pair[1] > 0)
        for x in range(6):
            at = pl.ds(z, 1)
            out_x[x, y, at, :] = out_x[x, y, at, :] + f_e[0, n, pl.ds(x, 1), :]
    receive(faces_yx)
    for side in range(2):
        for x in range(6):
            out_x[x, 6 * side] = out_x[x, 6 * side] + f_yx[side, x]
    for copy in copies:
        copy.wait_send()


def put_out(in_x, in_y, in_z, out_x, out_y, out_z, sem):
    pairs = ((in_x, out_x), (in_y, out_y), (in_z, out_z))
    copies = [pltpu.make_async_copy(*pair, sem.at[n]) for n, pair in enumerate(pairs)]
    for copy in copies:
        copy.start()
    for copy in copies:
        copy.wait()


def on_device(sizes, vectors, orient_flip, reluctivity, conductivity):
    f32 = jnp.float32
    regs = lambda n: pltpu.VMEM((n, 8, LANES), f32)
    grid = ((6, 7, 7, LANES), (7, 6, 7, LANES), (7, 6, 7, LANES))
    faces = [
        pltpu.VMEM(shape, f32)
        for shape in (
            (2, 6, 7, LANES),
            (2, 6, 7, LANES),
            (2, 6, 7, LANES),
            (2, 7, 6, LANES),
            (2, 6, 7, LANES),
            (2, 7, 6, LANES),
            (3, 4, 6, LANES),
        )
    ]
    results = pl.pallas_call(
        lambda *refs: kernel(sizes, *refs),
        out_shape=[pltpu.VMEM(shape, f32) for shape in grid],
        in_specs=[pl.BlockSpec(memory_space=pl.ANY)] * 4,
        out_specs=[pl.BlockSpec(memory_space=pltpu.VMEM)] * 3,
        scratch_shapes=[
            pltpu.VMEM((3, 6, 6, 6, LANES), f32),
            pltpu.VMEM(orient_flip.shape, jnp.int32),
            pltpu.VMEM(reluctivity.shape, f32),
            pltpu.VMEM(conductivity.shape, f32),
            pltpu.VMEM((8, 512), f32),
            regs(DOFS),
            regs(QPTS),
            regs(QPTS),
            pltpu.VMEM((8 * DOFS, LANES), f32),
            regs(QPTS),
            regs(QPTS),
            regs(QPTS),
            regs(QPTS),
            regs(QPTS),
            regs(QPTS),
            pltpu.VMEM((2, 6, 6, LANES), f32),
            pltpu.VMEM((2, 6, LANES), f32),
            pltpu.VMEM((2, 6, 6, LANES), f32),
            pltpu.VMEM((2, 6, 6, LANES), f32),
            pltpu.VMEM((2, 6, 6, LANES), f32),
            pltpu.VMEM((3, 6, LANES), f32),
            *[regs(QPTS)] * 4,
            *faces,
            *faces,
            pltpu.SemaphoreType.DMA((4,)),
            pltpu.SemaphoreType.DMA((31,)),
            pltpu.SemaphoreType.DMA((31,)),
        ],
        compiler_params=pltpu.CompilerParams(collective_id=0, has_side_effects=True),
        name="curlcurl",
    )(vectors, orient_flip, reluctivity, conductivity)
    results = [pltpu.with_memory_space_constraint(result, pltpu.VMEM) for result in results]
    out_x, out_y, out_z = pl.pallas_call(
        put_out,
        out_shape=[jax.ShapeDtypeStruct(shape, f32) for shape in grid],
        in_specs=[pl.BlockSpec(memory_space=pltpu.VMEM)] * 3,
        out_specs=[pl.BlockSpec(memory_space=pl.ANY)] * 3,
        scratch_shapes=[pltpu.SemaphoreType.DMA((3,))],
        name="putout",
    )(*results)
    return (out_x, out_y, jnp.swapaxes(out_z, 1, 2))


def solution(mesh):
    sizes = tuple(mesh.shape[axis] for axis in AXES)
    return jax.shard_map(
        lambda *args: on_device(sizes, *args),
        mesh=mesh,
        in_specs=(
            P(None, "gx", "gy", "gz", None),
            P("gx", "gy", "gz"),
            P("gx", "gy", "gz"),
            P("gx", "gy", "gz"),
        ),
        out_specs=(P("gx", "gy", "gz", None), P("gx", "gy", "gz", None), P("gx", "gy", "gz", None)),
        check_vma=False,
    )
```

```python
import jax
import jax.numpy as jnp
import numpy as np
from jax import lax
from jax.experimental import pallas as pl
from jax.experimental.pallas import tpu as pltpu
from jax.sharding import PartitionSpec as P

MESH = pl.DeviceIdType.MESH
AXES = ("gx", "gy", "gz")
LANES = 128
DOFS = 144
QPTS = 64
BASE = (0, 48, 96)
STRIDE = ((16, 4, 1), (12, 4, 1), (12, 3, 1))
EDGE_AXES = ((1, 2), (0, 2), (0, 1))
SIGNS = ((-1, -1), (-1, 1), (1, -1), (1, 1))


def lagrange(points_at, evaluate_at):
    amount = len(points_at)
    values = np.ones((len(evaluate_at), amount))
    slopes = np.zeros((len(evaluate_at), amount))
    for which in range(amount):
        for column in range(amount):
            if column != which:
                factor = (evaluate_at - points_at[column]) / (points_at[which] - points_at[column])
                slopes[:, which] = slopes[:, which] * factor + values[:, which] / (
                    points_at[which] - points_at[column]
                )
                values[:, which] = values[:, which] * factor
    return (values, slopes)


def basis_tables():
    lobatto = np.array([0.0, (1 - 5 ** (-0.5)) / 2, (1 + 5 ** (-0.5)) / 2, 1.0])
    gauss_open = np.array([(1 - 0.6**0.5) / 2, 0.5, (1 + 0.6**0.5) / 2])
    inner_pt = (3.0 / 7 - 2.0 / 7 * (6.0 / 5) ** 0.5) ** 0.5
    outer_pt = (3.0 / 7 + 2.0 / 7 * (6.0 / 5) ** 0.5) ** 0.5
    inner_wt = (18 + 30**0.5) / 36
    outer_wt = (18 - 30**0.5) / 36
    quad_points = (1 + np.array([-outer_pt, -inner_pt, inner_pt, outer_pt])) / 2
    quad_weight = np.array([outer_wt, inner_wt, inner_wt, outer_wt]) / 2
    closed, slopes = lagrange(lobatto, quad_points)
    opened, unused_slopes = lagrange(gauss_open, quad_points)
    return (closed, slopes, opened, quad_weight)


CLOSED, SLOPES, OPENED, WEIGHT = basis_tables()
DERIV = SLOPES @ np.linalg.inv(CLOSED)
OUTER, INNER = (0,), (1,)


def apply(table, given, parity, pairs=None):
    rows, columns = table.shape
    half = columns // 2
    sums = [given[c] + given[columns - 1 - c] for c in range(half)]
    diffs = [given[c] - given[columns - 1 - c] for c in range(half)]
    result = [None] * rows
    for q in pairs or range((rows + 1) // 2):
        even = None
        for c in range(half):
            term = sums[c] * float((table[q, c] + table[q, columns - 1 - c]) / 2)
            even = term if even is None else even + term
        if columns % 2:
            even = even + given[half] * float(table[q, half])
        if 2 * q + 1 == rows:
            result[q] = even
            continue
        odd = None
        for c in range(half):
            term = diffs[c] * float((table[q, c] - table[q, columns - 1 - c]) / 2)
            odd = term if odd is None else odd + term
        result[q] = even + odd
        result[rows - 1 - q] = even - odd if parity > 0 else odd - even
    return result


def along_rows(table, plane, parity=1, pairs=None):
    columns = [
        apply(table, [row[c] for row in plane], parity, pairs) for c in range(len(plane[0]))
    ]
    return [[column[q] for column in columns] for q in range(table.shape[0])]


def along_columns(table, plane, parity=1, pairs=None):
    return [apply(table, row, parity, pairs) for row in plane]


def combine(op, *planes):
    return [[op(*entries) for entries in zip(*rows)] for rows in zip(*planes)]


def plus(p, q):
    return combine(lambda s, t: s + t, p, q)


def minus(p, q):
    return combine(lambda s, t: s - t, p, q)


def times(p, q):
    return combine(lambda s, t: s * t, p, q)


def dof(comp, a, b, c):
    s = STRIDE[comp]
    return BASE[comp] + a * s[0] + b * s[1] + c * s[2]


def row_of(comp, a, b, c, element=0):
    return 8 * dof(comp, a, b, c) + element


def element(i, j, k):
    return 4 * k + 2 * i + j


def places(comp, axis):
    if comp == axis:
        return [(g, g // 3, g % 3) for g in range(6)]
    return [(g, 0, g) for g in range(4)] + [(g, 1, g - 3) for g in range(3, 7)]


def owners(comp, axis):
    last = 6 if comp == axis else 7
    return [(g, min(g // 3, 1), g - 3 * min(g // 3, 1)) for g in range(last)]


def prepare(flip, rel, con, flat, sign, mass, curl):
    for k in range(2):
        for i in range(2):
            at = pl.ds(4 * k + 2 * i, 2)
            flat[at, 0:DOFS] = 1.0 - 2.0 * flip[i][:, DOFS * k : DOFS * (k + 1)].astype(jnp.float32)
            flat[at, 256 : 256 + QPTS] = rel[i][:, QPTS * k : QPTS * (k + 1)]
            flat[at, 384 : 384 + QPTS] = con[i][:, QPTS * k : QPTS * (k + 1)]
    whole = flat[:, 0:DOFS]
    for d in range(DOFS):
        sign[d] = jnp.broadcast_to(whole[:, d : d + 1], (8, LANES))
    rel_all = flat[:, 256 : 256 + QPTS]
    con_all = flat[:, 384 : 384 + QPTS]
    for q in range(QPTS):
        weight = float(WEIGHT[q // 16] * WEIGHT[q // 4 % 4] * WEIGHT[q % 4])
        curl[q] = jnp.broadcast_to(rel_all[:, q : q + 1], (8, LANES)) * weight
        mass[q] = jnp.broadcast_to(con_all[:, q : q + 1], (8, LANES)) * weight


def quad(x, y, z):
    return 16 * x + 4 * y + z


def planes(ref, at):
    return [[ref[at(p, q)] for q in range(4)] for p in range(4)]


def put(ref, at, plane):
    for p, row in enumerate(plane):
        for q, value in enumerate(row):
            if value is not None:
                ref[at(p, q)] = value


def load_plane(dofs, sign, rows):
    return [
        [dofs[pl.ds(pl.multiple_of(8 * d, 8), 8), :] * sign[d] for d in row] for row in rows
    ]


def store_plane(dofs, sign, rows, plane):
    for row, values in zip(rows, plane):
        for d, value in zip(row, values):
            dofs[pl.ds(pl.multiple_of(8 * d, 8), 8), :] = value * sign[d]


def rows_fixed_b(comp, b):
    return [[dof(comp, a, b, c) for c in range(4 - (comp == 2))] for a in range(4 - (comp == 0))]


def rows_fixed_a(comp, a):
    return [[dof(comp, a, b, c) for c in range(4)] for b in range(3)]


def forward_y(dofs, sign, temp, u_y, c_x, c_z):
    @pl.loop(0, 4, unroll=True)
    def _(a):
        values = along_rows(OPENED, load_plane(dofs, sign, rows_fixed_a(1, a)))
        put(temp, lambda y, z: quad(a, y, z), along_columns(CLOSED, values))

    @pl.loop(0, 4, unroll=True)
    def _(y):
        at = lambda x, z: quad(x, y, z)
        u = along_rows(CLOSED, planes(temp, at))
        put(u_y, at, u)
        put(c_z, at, along_rows(DERIV, u, -1))
        put(c_x, at, along_columns(-DERIV, u, -1))


def start_x(dofs, sign, temp, b):
    values = along_rows(OPENED, load_plane(dofs, sign, rows_fixed_b(0, b)))
    put(temp, lambda x, z: quad(x, b, z), along_columns(CLOSED, values))


def start_z(dofs, sign, temp, b):
    values = along_columns(OPENED, load_plane(dofs, sign, rows_fixed_b(2, b)))
    put(temp, lambda x, z: quad(x, b, z), along_rows(CLOSED, values))


def forward_x(temp, curl, u_x, c_y, c_z):
    @pl.loop(0, 4, unroll=True)
    def _(x):
        at = lambda y, z: quad(x, y, z)
        u = along_rows(CLOSED, planes(temp, at))
        put(u_x, at, u)
        w_z = minus(planes(c_z, at), along_rows(DERIV, u, -1))
        put(c_z, at, times(planes(curl, at), w_z))
        put(c_y, at, along_columns(DERIV, u, -1))


def turn_z(temp, kept, mass, curl, c_x, c_y):
    @pl.loop(0, 4, unroll=True)
    def _(z):
        at = lambda x, y: quad(x, y, z)
        u = along_columns(CLOSED, planes(temp, at))
        scale = planes(curl, at)
        w_y = times(scale, minus(planes(c_y, at), along_rows(DERIV, u, -1)))
        w_x = times(scale, plus(planes(c_x, at), along_columns(DERIV, u, -1)))
        put(c_y, at, w_y)
        put(c_x, at, w_x)
        v = times(planes(mass, at), u)
        v = plus(v, along_columns(DERIV.T, w_x, -1))
        v = minus(v, along_rows(DERIV.T, w_y, -1))
        put(kept, at, v)
        put(temp, at, along_columns(CLOSED.T, v, 1, OUTER))


def inner_z(temp, kept):
    @pl.loop(0, 4, unroll=True)
    def _(z):
        at = lambda x, y: quad(x, y, z)
        put(temp, at, along_columns(CLOSED.T, planes(kept, at), 1, INNER))


def finish_z(dofs, sign, temp, first, last, step):
    @pl.loop(first, last, step=step, unroll=True)
    def _(b):
        values = along_rows(CLOSED.T, planes(temp, lambda x, z: quad(x, b, z)))
        store_plane(dofs, sign, rows_fixed_b(2, b), along_columns(OPENED.T, values))


def backward_x(mass, temp, kept, u_x, c_y, c_z):
    @pl.loop(0, 4, unroll=True)
    def _(x):
        at = lambda y, z: quad(x, y, z)
        v = times(planes(mass, at), planes(u_x, at))
        v = plus(v, along_columns(DERIV.T, planes(c_y, at), -1))
        v = minus(v, along_rows(DERIV.T, planes(c_z, at), -1))
        put(kept, at, v)
        put(temp, at, along_rows(CLOSED.T, v, 1, OUTER))


def inner_x(temp, kept):
    @pl.loop(0, 4, unroll=True)
    def _(x):
        at = lambda y, z: quad(x, y, z)
        put(temp, at, along_rows(CLOSED.T, planes(kept, at), 1, INNER))


def finish_x(dofs, sign, temp, first, last, step):
    @pl.loop(first, last, step=step, unroll=True)
    def _(b):
        values = along_columns(CLOSED.T, planes(temp, lambda x, z: quad(x, b, z)))
        store_plane(dofs, sign, rows_fixed_b(0, b), along_rows(OPENED.T, values))


def backward_y(dofs, sign, mass, temp, u_y, c_x, c_z):
    @pl.loop(0, 4, unroll=True)
    def _(y):
        at = lambda x, z: quad(x, y, z)
        v = times(planes(mass, at), planes(u_y, at))
        v = plus(v, along_rows(DERIV.T, planes(c_z, at), -1))
        v = minus(v, along_columns(DERIV.T, planes(c_x, at), -1))
        put(temp, at, along_rows(CLOSED.T, v))

    @pl.loop(0, 4, unroll=True)
    def _(a):
        values = along_columns(CLOSED.T, planes(temp, lambda y, z: quad(a, y, z)))
        store_plane(dofs, sign, rows_fixed_a(1, a), along_rows(OPENED.T, values))


def join_elements(dofs, comp, axes=(0, 1, 2), only_b=None):
    rows = lax.broadcasted_iota(jnp.int32, (8, LANES), 0)
    for axis, step in ((0, 2), (1, 1), (2, 4)):
        if comp == axis or axis not in axes:
            continue
        upper = (rows // step) % 2 == 1
        sizes = [range(3 if comp == other else 4) for other in range(3)]
        sizes[axis] = range(1)
        if only_b:
            sizes[1] = only_b
        for a in sizes[0]:
            for b in sizes[1]:
                for c in sizes[2]:
                    high = [a, b, c]
                    high[axis] = 3
                    to = pl.ds(row_of(comp, a, b, c), 8)
                    moved = pltpu.roll(dofs[pl.ds(row_of(comp, *high), 8), :], step, 0)
                    dofs[to, :] = dofs[to, :] + jnp.where(upper, moved, 0.0)


def scatter_own(vec, dofs):
    for comp in range(3):
        for x, i, a in places(comp, 0):
            for y, j, b in places(comp, 1):
                if x == 6 or y == 6:
                    continue
                for k in range(2):
                    count = 4 if comp != 2 and k == 0 else 3
                    at = row_of(comp, a, b, 0, element(i, j, k))
                    dofs[pl.ds(at, count, 8), :] = vec[comp, x, y, pl.ds(3 * k, count), :]


def scatter_line(dofs, comp, i, a, j, b, source):
    for k in range(2):
        count = 4 if comp != 2 and k == 0 else 3
        at = row_of(comp, a, b, 0, element(i, j, k))
        dofs[pl.ds(at, count, 8), :] = source(pl.ds(3 * k, count))


def scatter_xz_halo(dofs, r_x, r_z):
    for comp in (1, 2):
        for y, j, b in places(comp, 1):
            if y < 6:
                scatter_line(dofs, comp, 1, 3, j, b, lambda z: r_x[comp - 1, y, z, :])
    for x, i, a in places(0, 0):
        for j in range(2):
            count = 4 - j
            at = row_of(0, a, 0, 3, element(i, j, 1))
            dofs[pl.ds(at, count, 32), :] = r_z[0, x, pl.ds(3 * j, count), :]
    for x, i, a in places(1, 0):
        if x < 6:
            for j in range(2):
                at = row_of(1, a, 0, 3, element(i, j, 1))
                dofs[pl.ds(at, 3, 32), :] = r_z[1, x, pl.ds(3 * j, 3), :]


def scatter_xz_edge(dofs, r_e):
    for j in range(2):
        at = row_of(1, 3, 0, 3, element(1, j, 1))
        dofs[pl.ds(at, 3, 32), :] = r_e[1, pl.ds(3 * j, 3), :]


def scatter_y_halo(dofs, r_y, r_e):
    for comp in (0, 2):
        for x, i, a in places(comp, 0):
            if x < 6:
                scatter_line(dofs, comp, i, a, 1, 3, lambda z: r_y[comp // 2, x, z, :])
    for i in range(2):
        at = row_of(0, 0, 3, 3, element(i, 1, 1))
        dofs[pl.ds(at, 3, 128), :] = r_e[0, pl.ds(3 * i, 3), :]


def runs(comp, axis, fixed):
    local = [None if g is None else owners(comp, n)[g][1:] for n, g in enumerate(fixed)]
    result = []
    for half in range(2):
        count = 3 + half * (comp != axis)
        at = [(half, 0) if entry is None else entry for entry in local]
        (i, a), (j, b), (k, c) = at
        row = row_of(comp, a, b, c, element(i, j, k))
        result.append((pl.ds(3 * half, count), pl.ds(row, count, 8 * STRIDE[comp][axis])))
    return result


def owned(comp, axis):
    return range(6 if comp == axis else 7)


def to_grid(dofs, comp, out, line):
    other = 3 - line
    for x in owned(comp, 0):
        for q in owned(comp, other):
            fixed = [x, None, None]
            fixed[other] = q
            for grid, rows in runs(comp, line, fixed):
                out[x, q, grid, :] = dofs[rows, :]


def pack_face(dofs, comp, axis, line, pack):
    third = 3 - axis - line
    for side in range(2):
        for p in owned(comp, third):
            fixed = [None] * 3
            fixed[axis] = 6 * side
            fixed[third] = p
            for grid, rows in runs(comp, line, fixed):
                pack[side, p, grid, :] = dofs[rows, :]


def add_face(dofs, comp, axis, line, given):
    third = 3 - axis - line
    for side in range(2):
        for p in owned(comp, third):
            fixed = [None] * 3
            fixed[axis] = 6 * side
            fixed[third] = p
            for grid, rows in runs(comp, line, fixed):
                dofs[rows, :] = dofs[rows, :] + given[side, p, grid, :]


def edge_runs(comp, n):
    fixed = [None] * 3
    for axis, sign in zip(EDGE_AXES[comp], SIGNS[n]):
        fixed[axis] = 6 * (sign > 0)
    return runs(comp, comp, fixed)


def pack_edges(dofs, comp, edges):
    for n in range(4):
        for grid, rows in edge_runs(comp, n):
            edges[comp, n, grid, :] = dofs[rows, :]


def add_edges(dofs, comp, given):
    for n in range(4):
        for grid, rows in edge_runs(comp, n):
            dofs[rows, :] = dofs[rows, :] + given[comp, n, grid, :]


def kernel(
    sizes,
    vec_hbm,
    flip_hbm,
    rel_hbm,
    con_hbm,
    out_x,
    out_y,
    out_z,
    vec,
    flip,
    rel,
    con,
    flat,
    sign,
    mass,
    curl,
    dofs,
    temp,
    u_x,
    u_y,
    c_x,
    c_y,
    c_z,
    s_z,
    s_e,
    r_x,
    r_y,
    r_z,
    r_e,
    t_x,
    t_z,
    v_x,
    v_z,
    p_xy,
    p_xz,
    p_yx,
    p_yz,
    p_zx,
    p_zy,
    p_e,
    f_xy,
    f_xz,
    f_yx,
    f_yz,
    f_zx,
    f_zy,
    f_e,
    load_sem,
    send_sem,
    recv_sem,
):
    me = [lax.axis_index(axis) for axis in AXES]

    def neighbour(*steps):
        return tuple(lax.rem(me[n] + steps[n] + sizes[n], sizes[n]) for n in range(3))

    loads = [
        pltpu.make_async_copy(source, target, load_sem.at[n])
        for n, (source, target) in enumerate(
            ((vec_hbm, vec), (flip_hbm, flip), (rel_hbm, rel), (con_hbm, con))
        )
    ]
    for copy in loads:
        copy.start()

    barrier = pltpu.get_barrier_semaphore()
    upper = ((0, 1, 0), (1, 1, 0), (0, 1, 1), (1, 0, 0), (1, 0, 1), (0, 0, 1))
    for steps in upper:
        pl.semaphore_signal(barrier, inc=1, device_id=neighbour(*steps), device_id_type=MESH)

    copies = []

    def send(source, target, *steps):
        n = len(copies)
        copy = pltpu.make_async_remote_copy(
            src_ref=source,
            dst_ref=target,
            send_sem=send_sem.at[n],
            recv_sem=recv_sem.at[n],
            device_id=neighbour(*steps),
            device_id_type=MESH,
        )
        copy.start()
        copies.append(copy)
        return copy

    def send_faces(axis, pack, target):
        faces = []
        for side in (1, 0):
            steps = [(2 * side - 1) * (axis == n) for n in range(3)]
            faces.append(send(pack.at[side], target.at[1 - side], *steps))
        return faces

    def send_edges(comp):
        sent = []
        for n, pair in reversed(tuple(enumerate(SIGNS))):
            steps = [0, 0, 0]
            for axis, step in zip(EDGE_AXES[comp], pair):
                steps[axis] = step
            sent.append(send(p_e.at[comp, n], f_e.at[comp, 3 - n], *steps))
        return sent

    def receive(arriving):
        for copy in arriving:
            copy.wait_recv()

    loads[0].wait()
    for comp in range(2):
        for x in range(6):
            for y in range(6):
                s_z[comp, x, pl.ds(y, 1), :] = vec[comp, x, y, pl.ds(0, 1), :]
    for n in range(6):
        s_e[0, pl.ds(n, 1), :] = vec[0, n, 0, pl.ds(0, 1), :]
        s_e[1, pl.ds(n, 1), :] = vec[1, 0, n, pl.ds(0, 1), :]
    scatter_own(vec, dofs)
    pl.semaphore_wait(barrier, len(upper))
    xy_halo = [send(vec.at[2, 0, 0], r_e.at[2], -1, -1, 0)]
    y_halo = [
        send(s_e.at[0], r_e.at[0], 0, -1, -1),
        send(vec.at[0, :, 0], r_y.at[0], 0, -1, 0),
        send(vec.at[2, :, 0], r_y.at[1], 0, -1, 0),
    ]
    xz_halo = [
        send(s_e.at[1], r_e.at[1], -1, 0, -1),
        send(vec.at[pl.ds(1, 2), 0], r_x, -1, 0, 0),
        send(s_z, r_z, 0, 0, -1),
    ]

    for copy in loads[1:]:
        copy.wait()
    prepare(flip, rel, con, flat, sign, mass, curl)
    receive(xz_halo[1:])
    scatter_xz_halo(dofs, r_x, r_z)

    @pl.loop(0, 3, unroll=1)
    def _(b):
        start_x(dofs, sign, t_x, b)
        start_z(dofs, sign, t_z, b)

    receive(xz_halo[:1])
    scatter_xz_edge(dofs, r_e)
    forward_y(dofs, sign, temp, u_y, c_x, c_z)
    receive(y_halo)
    scatter_y_halo(dofs, r_y, r_e)
    start_x(dofs, sign, t_x, 3)
    forward_x(t_x, curl, u_x, c_y, c_z)
    receive(xy_halo)
    scatter_line(dofs, 2, 1, 3, 1, 3, lambda z: r_e[2, z, :])
    start_z(dofs, sign, t_z, 3)
    turn_z(t_z, v_z, mass, curl, c_x, c_y)
    finish_z(dofs, sign, t_z, 0, 4, 3)
    join_elements(dofs, 2, (0,), (0, 3))
    pack_edges(dofs, 2, p_e)
    edges_z = send_edges(2)
    pack_face(dofs, 2, 1, 2, p_yz)
    faces_yz = send_faces(1, p_yz, f_yz)

    backward_y(dofs, sign, mass, temp, u_y, c_x, c_z)
    join_elements(dofs, 1)
    pack_edges(dofs, 1, p_e)
    edges_y = send_edges(1)
    pack_face(dofs, 1, 0, 2, p_xy)
    faces_xy = send_faces(0, p_xy, f_xy)

    backward_x(mass, t_x, v_x, u_x, c_y, c_z)
    finish_x(dofs, sign, t_x, 0, 4, 3)
    join_elements(dofs, 0, (2,), (0, 3))
    pack_edges(dofs, 0, p_e)
    edges_x = send_edges(0)
    pack_face(dofs, 0, 1, 2, p_yx)
    faces_yx = send_faces(1, p_yx, f_yx)

    inner_z(t_z, v_z)
    finish_z(dofs, sign, t_z, 1, 3, 1)
    join_elements(dofs, 2, (0,), (1, 2))
    join_elements(dofs, 2, (1,))
    pack_face(dofs, 2, 0, 1, p_xz)
    faces_xz = send_faces(0, p_xz, f_xz)
    pack_face(dofs, 1, 2, 1, p_zy)
    faces_zy = send_faces(2, p_zy, f_zy)
    inner_x(t_x, v_x)
    finish_x(dofs, sign, t_x, 1, 3, 1)
    join_elements(dofs, 0, (2,), (1, 2))
    join_elements(dofs, 0, (1,))
    pack_face(dofs, 0, 2, 1, p_zx)
    faces_zx = send_faces(2, p_zx, f_zx)

    receive(faces_zy + edges_y)
    add_face(dofs, 1, 2, 1, f_zy)
    add_edges(dofs, 1, f_e)
    to_grid(dofs, 1, out_y, 2)
    receive(faces_xy)
    for side in range(2):
        out_y[6 * side] = out_y[6 * side] + f_xy[side]
    receive(faces_zx)
    add_face(dofs, 0, 2, 1, f_zx)
    to_grid(dofs, 0, out_x, 2)
    receive(faces_yz + edges_z)
    add_face(dofs, 2, 1, 2, f_yz)
    add_edges(dofs, 2, f_e)
    to_grid(dofs, 2, out_z, 1)
    receive(faces_xz)
    for side in range(2):
        out_z[6 * side] = out_z[6 * side] + f_xz[side]
    receive(edges_x)
    for n, pair in enumerate(SIGNS):
        y, z = 6 * (pair[0] > 0), 6 * (pair[1] > 0)
        for x in range(6):
            at = pl.ds(z, 1)
            out_x[x, y, at, :] = out_x[x, y, at, :] + f_e[0, n, pl.ds(x, 1), :]
    receive(faces_yx)
    for side in range(2):
        for x in range(6):
            out_x[x, 6 * side] = out_x[x, 6 * side] + f_yx[side, x]
    for copy in copies:
        copy.wait_send()


def put_out(in_x, in_y, in_z, out_x, out_y, out_z, sem):
    pairs = ((in_x, out_x), (in_y, out_y), (in_z, out_z))
    copies = [pltpu.make_async_copy(*pair, sem.at[n]) for n, pair in enumerate(pairs)]
    for copy in copies:
        copy.start()
    for copy in copies:
        copy.wait()


def on_device(sizes, vectors, orient_flip, reluctivity, conductivity):
    f32 = jnp.float32
    regs = lambda n: pltpu.VMEM((n, 8, LANES), f32)
    grid = ((6, 7, 7, LANES), (7, 6, 7, LANES), (7, 6, 7, LANES))
    faces = [
        pltpu.VMEM(shape, f32)
        for shape in (
            (2, 6, 7, LANES),
            (2, 6, 7, LANES),
            (2, 6, 7, LANES),
            (2, 7, 6, LANES),
            (2, 6, 7, LANES),
            (2, 7, 6, LANES),
            (3, 4, 6, LANES),
        )
    ]
    results = pl.pallas_call(
        lambda *refs: kernel(sizes, *refs),
        out_shape=[pltpu.VMEM(shape, f32) for shape in grid],
        in_specs=[pl.BlockSpec(memory_space=pl.ANY)] * 4,
        out_specs=[pl.BlockSpec(memory_space=pltpu.VMEM)] * 3,
        scratch_shapes=[
            pltpu.VMEM((3, 6, 6, 6, LANES), f32),
            pltpu.VMEM(orient_flip.shape, jnp.int32),
            pltpu.VMEM(reluctivity.shape, f32),
            pltpu.VMEM(conductivity.shape, f32),
            pltpu.VMEM((8, 512), f32),
            regs(DOFS),
            regs(QPTS),
            regs(QPTS),
            pltpu.VMEM((8 * DOFS, LANES), f32),
            regs(QPTS),
            regs(QPTS),
            regs(QPTS),
            regs(QPTS),
            regs(QPTS),
            regs(QPTS),
            pltpu.VMEM((2, 6, 6, LANES), f32),
            pltpu.VMEM((2, 6, LANES), f32),
            pltpu.VMEM((2, 6, 6, LANES), f32),
            pltpu.VMEM((2, 6, 6, LANES), f32),
            pltpu.VMEM((2, 6, 6, LANES), f32),
            pltpu.VMEM((3, 6, LANES), f32),
            *[regs(QPTS)] * 4,
            *faces,
            *faces,
            pltpu.SemaphoreType.DMA((4,)),
            pltpu.SemaphoreType.DMA((31,)),
            pltpu.SemaphoreType.DMA((31,)),
        ],
        compiler_params=pltpu.CompilerParams(collective_id=0, has_side_effects=True),
        name="curlcurl",
    )(vectors, orient_flip, reluctivity, conductivity)
    results = [pltpu.with_memory_space_constraint(result, pltpu.VMEM) for result in results]
    out_x, out_y, out_z = pl.pallas_call(
        put_out,
        out_shape=[jax.ShapeDtypeStruct(shape, f32) for shape in grid],
        in_specs=[pl.BlockSpec(memory_space=pltpu.VMEM)] * 3,
        out_specs=[pl.BlockSpec(memory_space=pl.ANY)] * 3,
        scratch_shapes=[pltpu.SemaphoreType.DMA((3,))],
        name="putout",
    )(*results)
    return (out_x, out_y, jnp.swapaxes(out_z, 1, 2))


def solution(mesh):
    sizes = tuple(mesh.shape[axis] for axis in AXES)
    return jax.shard_map(
        lambda *args: on_device(sizes, *args),
        mesh=mesh,
        in_specs=(
            P(None, "gx", "gy", "gz", None),
            P("gx", "gy", "gz"),
            P("gx", "gy", "gz"),
            P("gx", "gy", "gz"),
        ),
        out_specs=(P("gx", "gy", "gz", None), P("gx", "gy", "gz", None), P("gx", "gy", "gz", None)),
        check_vma=False,
    )
```
